8 devices in a mesh: nodes: 8 (over z, y, x, core).
Axes of the slice: x: 2, y: 2, z: 1, core: 2. Of those that a mesh axis runs over, the one named last changes fastest.
Arguments:
- adjacency: bfloat16 [16384, 16384], P('nodes')
- features: bfloat16 [16384, 100], P('nodes')
- w_one: float32 [100, 128], replicated
- w_two: float32 [128, 47], replicated
- labels: int32 [16384], P('nodes')
- label_mask: int32 [16384], P('nodes')
Outputs:
- output 1: float32 [1], replicated
- output 2: float32 [100, 128], replicated
- output 3: float32 [128, 47], replicated
All inputs are finite; a program needn't handle non-finite values.
Results may differ from the reference program's by a relative error of at most 0.001.
Values are sent between devices in bfloat16 or wider.
A program may use at most 1 GiB of HBM per device.

```python
import math
import jax
import jax.numpy as jnp
from jax import lax

NODES = 16384
BLOCK_ROWS = 2048
F_IN = 100
HIDDEN = 128
CLASSES = 47

ROW_CONTRACT = (((0,), (0,)), ((), ()))
COL_CONTRACT = (((1,), (1,)), ((), ()))


def setup_inputs(seed: int = 0) -> dict:
    key_list = jax.random.split(jax.random.key(seed), 8)
    num_comms = NODES // BLOCK_ROWS
    shifts = jax.random.randint(key_list[0], (2,), 1, num_comms)
    col_ids = jnp.arange(NODES)
    col_comm = col_ids // BLOCK_ROWS
    row_ids = jnp.arange(BLOCK_ROWS)

    def draw_rows(block_idx):
        hot_cols = (col_comm == (block_idx + shifts[0]) % num_comms) | (col_comm == (block_idx + shifts[1]) % num_comms)
        edge_prob = jnp.where(hot_cols, 0.5, 0.01)
        coin_flip = jax.random.uniform(jax.random.fold_in(key_list[1], block_idx), (BLOCK_ROWS, NODES))
        self_loop = col_ids[None, :] == block_idx * BLOCK_ROWS + row_ids[:, None]
        raw_edges = jnp.where((coin_flip < edge_prob[None, :]) | self_loop, 1.0, 0.0)
        return (raw_edges / jnp.sum(raw_edges, axis=1, keepdims=True)).astype(jnp.bfloat16)

    adjacency = lax.map(draw_rows, jnp.arange(num_comms)).reshape(NODES, NODES)
    centers = jax.random.normal(key_list[2], (num_comms, F_IN))
    feat_noise = jax.random.normal(key_list[3], (NODES, F_IN))
    features = (jnp.repeat(centers, BLOCK_ROWS, axis=0) + feat_noise).astype(jnp.bfloat16)
    w_one = jax.random.normal(key_list[4], (F_IN, HIDDEN)) * math.sqrt(2.0 / F_IN)
    w_two = jax.random.normal(key_list[5], (HIDDEN, CLASSES)) * (2.0 / math.sqrt(HIDDEN))
    labels = jax.random.randint(key_list[6], (NODES,), 0, CLASSES, dtype=jnp.int32)
    drawn_mask = jax.random.randint(key_list[7], (NODES,), 0, 10, dtype=jnp.int32) < 3
    label_mask = jnp.where((jnp.arange(NODES) % 10 == 0) | drawn_mask, 1, 0).astype(jnp.int32)
    return {'adjacency': adjacency, 'features': features, 'w_one': w_one.astype(jnp.float32), 'w_two': w_two.astype(jnp.float32), 'labels': labels, 'label_mask': label_mask}


def reference(adjacency, features, w_one, w_two, labels, label_mask):
    weight_one = w_one.astype(jnp.bfloat16)
    weight_two = w_two.astype(jnp.bfloat16)
    agg_one = jnp.dot(adjacency, features, preferred_element_type=jnp.float32).astype(jnp.bfloat16)
    pre_one = jnp.dot(agg_one, weight_one, preferred_element_type=jnp.float32)
    hidden = jnp.maximum(pre_one, 0.0).astype(jnp.bfloat16)
    agg_two = jnp.dot(adjacency, hidden, preferred_element_type=jnp.float32).astype(jnp.bfloat16)
    logits = jnp.dot(agg_two, weight_two, preferred_element_type=jnp.float32)
    weight = label_mask.astype(jnp.float32)
    label_count = jnp.sum(weight)
    onehot = (labels[:, None] == jnp.arange(CLASSES)[None, :]).astype(jnp.float32)
    log_prob = jax.nn.log_softmax(logits, axis=-1)
    loss_value = -jnp.sum(weight * jnp.sum(onehot * log_prob, axis=-1)) / label_count
    grad_two = (weight[:, None] * (jnp.exp(log_prob) - onehot) / label_count).astype(jnp.bfloat16)
    dw_two = lax.dot_general(agg_two, grad_two, ROW_CONTRACT, preferred_element_type=jnp.float32)
    back_two = lax.dot_general(grad_two, weight_two, COL_CONTRACT, preferred_element_type=jnp.float32).astype(jnp.bfloat16)
    d_hidden = lax.dot_general(adjacency, back_two, ROW_CONTRACT, preferred_element_type=jnp.float32)
    grad_one = jnp.where(pre_one > 0.0, d_hidden, 0.0).astype(jnp.bfloat16)
    dw_one = lax.dot_general(agg_one, grad_one, ROW_CONTRACT, preferred_element_type=jnp.float32)
    return (loss_value.reshape(1), dw_one, dw_two)
```

```python
import jax
import jax.numpy as jnp
from jax import lax
from jax.experimental import pallas as pl
from jax.experimental.pallas import tpu as pltpu
from jax.sharding import PartitionSpec as P

MESH = pl.DeviceIdType.MESH
F32, BF16 = jnp.float32, jnp.bfloat16
LANE_CONTRACT = (((1,), (1,)), ((), ()))

ROWS = 2048
TILE = 1024
SLOTS = 8
FEAT = 104
HID = 128
CLS = 48
RED = FEAT + CLS + 8


def kernel(adj, feat, w1t, w2t, w2, label, mask, mask_any, out,
           ring, xbuf, sbuf, acc1, acc2, hid, s2t, ut, mall, dcls,
           pbuf, rbuf, cbuf, rsbuf, red, redp, half, fin,
           ring_sem, loc_sem, ag_send, ag_recv, m_send, m_recv,
           d_send, d_recv, rs_send, rs_recv, f_send, f_recv):
    me = lax.axis_index('nodes')
    core, px, py = me % 2, (me // 2) % 2, me // 4

    def device(fy, fx, fc):
        return 4 * ((py + fy) % 2) + 2 * ((px + fx) % 2) + (core + fc) % 2

    partner, xn, yn, diag = device(0, 0, 1), device(0, 1, 0), device(1, 0, 0), device(1, 1, 0)

    def columns(u):
        s, back = u % 16, u // 32
        g = (1 - back) * (s // 4) + back * (3 - s // 4)
        r = (1 - back) * (s % 2) + back * ((s // 2) % 2)
        fc = (1 - back) * ((s // 2) % 2) + back * (1 - s % 2)
        t = (g + 1) // 2
        fx, fy = (t + 1 - r) // 2, (t + r) // 2
        h = (r + (g // 2) * (3 - g)) % 2
        return pl.multiple_of(device(fy, fx, fc) * ROWS + h * TILE, TILE)

    def tile(u):
        slot = u % SLOTS
        return pltpu.make_async_copy(adj.at[:, pl.ds(columns(u), TILE)], ring.at[slot], ring_sem.at[slot])

    def remote(src, dst, ssem, rsem, dev):
        return pltpu.make_async_remote_copy(src_ref=src, dst_ref=dst, send_sem=ssem, recv_sem=rsem,
                                            device_id=(dev,), device_id_type=MESH)

    for u in range(SLOTS):
        tile(u).start()
    own = [pltpu.make_async_copy(feat.at[:, pl.ds(h * TILE, TILE)], xbuf.at[h], loc_sem.at[h]) for h in range(2)]
    own.append(pltpu.make_async_copy(mask_any, mall.at[0], loc_sem.at[2]))
    for c in own:
        c.start()

    peers = [device(e // 4, (e // 2) % 2, e % 2) for e in range(8)]
    barrier = pltpu.get_barrier_semaphore()
    for e in range(1, 8):
        pl.semaphore_signal(barrier, inc=1, device_id=(peers[e],), device_id_type=MESH)
    pl.semaphore_wait(barrier, 7)

    def gather_copy(ph, buf, src, step, dev):
        return remote(src, buf.at[step], ag_send.at[ph, step], ag_recv.at[ph, step], dev)

    def gather_start(ph, buf, srcs):
        for step, h, dev in ((4, 0, xn), (5, 1, yn), (2, 0, partner), (3, 1, partner), (8, 1, xn), (9, 0, yn)):
            gather_copy(ph, buf, srcs[h], step, dev).start()

    def gather_step(ph, buf, s):
        @pl.when(s >= 2)
        def _():
            gather_copy(ph, buf, buf.at[s], s, partner).wait_recv()

        @pl.when((s >= 4) & (s % 4 < 2))
        def _():
            gather_copy(ph, buf, buf.at[s], s + 2, partner).start()

        @pl.when(s == 4)
        def _():
            gather_copy(ph, buf, buf.at[s], 12, yn).start()

        @pl.when(s == 5)
        def _():
            gather_copy(ph, buf, buf.at[s], 13, xn).start()

    def gather_finish(ph, buf):
        for step in range(2, 16):
            gather_copy(ph, buf, buf.at[0], step, partner).wait_send()

    gather_start(0, xbuf, [feat.at[:, pl.ds(h * TILE, TILE)] for h in range(2)])
    m_copies = [remote(mask_any, mall.at[e], m_send.at[e], m_recv.at[e], peers[e]) for e in range(1, 8)]
    for c in m_copies:
        c.start()
    for c in own:
        c.wait()

    acc1[...] = jnp.zeros_like(acc1)

    def first(s, _):
        tile(s).wait()
        gather_step(0, xbuf, s)
        acc1[...] += lax.dot_general(xbuf[s], ring[s % SLOTS], LANE_CONTRACT, preferred_element_type=F32)
        tile(s + SLOTS).start()
        return 0

    lax.fori_loop(0, 16, first, 0)
    for h in range(2):
        sbuf[h] = acc1[:, h * TILE:(h + 1) * TILE].astype(BF16)
    gather_start(1, sbuf, [sbuf.at[h] for h in range(2)])

    acc2[...] = jnp.zeros_like(acc2)

    def second(s, _):
        tile(s + 16).wait()
        gather_step(1, sbuf, s)
        hid[...] = jnp.maximum(jnp.dot(w1t[...], sbuf[s], preferred_element_type=F32), 0.0).astype(BF16)
        acc2[...] += lax.dot_general(hid[...], ring[s % SLOTS], LANE_CONTRACT, preferred_element_type=F32)
        tile(s + 16 + SLOTS).start()
        return 0

    lax.fori_loop(0, 16, second, 0)

    for c in m_copies:
        c.wait()
    count = jnp.sum(jnp.sum(mall[...], axis=0))
    classes = lax.broadcasted_iota(jnp.int32, (CLS, 512), 0)

    def heads(i, loss):
        cols = pl.ds(pl.multiple_of(i * 512, 512), 512)
        agg = acc2[:, cols].astype(BF16)
        s2t[:, cols] = agg
        z = jnp.dot(w2t[...], agg, preferred_element_type=F32)
        z = jnp.where(classes < 47, z, -1e30)
        z = z - jnp.max(z, axis=0, keepdims=True)
        logp = z - jnp.log(jnp.sum(jnp.exp(z), axis=0, keepdims=True))
        onehot = (label[:, cols] == classes).astype(F32)
        weight = mask[:, cols]
        g2 = (weight * (jnp.exp(logp) - onehot) / count).astype(BF16)
        dcls[:, cols] = g2
        ut[:, cols] = jnp.dot(w2[...], g2, preferred_element_type=F32).astype(BF16)
        return loss + weight * jnp.sum(jnp.where(label[:, cols] == classes, logp, 0.0), axis=0, keepdims=True)

    loss = lax.fori_loop(0, ROWS // 512, heads, jnp.zeros((1, 512), F32))

    to_y = (True, False, False, True, False, True)

    def pair_copy(j):
        return remote(pbuf.at[j], rbuf.at[j], d_send.at[j], d_recv.at[j], partner)

    def link_copy(j):
        return remote(cbuf.at[j], rsbuf.at[j], rs_send.at[j], rs_recv.at[j], yn if to_y[j] else xn)

    def finalize(j):
        pair_copy(j).wait_recv()
        if j in (4, 5):
            link_copy(j - 4).wait_recv()
            cbuf[j] = (cbuf[j] + rbuf[j]) + rsbuf[j - 4]
        else:
            cbuf[j] = cbuf[j] + rbuf[j]
        if j < 6:
            link_copy(j).start()

    def third(j, _):
        u = 32 + 2 * j
        tile(u).wait()
        pbuf[j] = jnp.dot(ut[...], ring[u % SLOTS], preferred_element_type=F32)
        pair_copy(j).start()

        @pl.when(j < 4)
        def _():
            tile(u + SLOTS).start()

        tile(u + 1).wait()
        cbuf[j] = jnp.dot(ut[...], ring[(u + 1) % SLOTS], preferred_element_type=F32)

        @pl.when(j < 4)
        def _():
            tile(u + 1 + SLOTS).start()

        for jj in range(7):
            @pl.when(j == jj + 1)
            def _(jj=jj):
                finalize(jj)
        return 0

    lax.fori_loop(0, 8, third, 0)
    finalize(7)

    red[FEAT:FEAT + CLS, :] = lax.dot_general(dcls[...], s2t[...], LANE_CONTRACT, preferred_element_type=F32)
    red[FEAT + CLS:, :] = jnp.broadcast_to(-jnp.sum(loss), (8, HID))
    gather_finish(0, xbuf)
    gather_finish(1, sbuf)
    for j in range(8):
        pair_copy(j).wait_send()

    dw1 = jnp.zeros((FEAT, HID), F32)
    for h, (a, b) in enumerate(((3, 4), (2, 5))):
        z1 = jnp.dot(w1t[...], sbuf[h], preferred_element_type=F32)
        link_copy(a).wait_recv()
        link_copy(b).wait_recv()
        g1 = jnp.where(z1 > 0.0, (cbuf[6 + h] + rsbuf[a]) + rsbuf[b], 0.0).astype(BF16)
        dw1 = dw1 + lax.dot_general(sbuf[h], g1, LANE_CONTRACT, preferred_element_type=F32)
    red[:FEAT, :] = dw1
    for j in range(6):
        link_copy(j).wait_send()

    c0 = remote(red, redp, f_send.at[0], f_recv.at[0], partner)
    c0.start()
    c0.wait()
    rows = pl.ds(pl.multiple_of(core * (RED // 2), 8), RED // 2)
    half[0] = red[rows, :] + redp[rows, :]
    copies = [remote(half.at[0], half.at[e], f_send.at[e], f_recv.at[e], dev) for e, dev in ((1, xn), (2, yn), (3, diag))]
    for c in copies:
        c.start()
    for c in copies:
        c.wait()
    fin[rows, :] = (half[0] + half[1]) + (half[2] + half[3])
    c4 = remote(fin.at[rows], fin.at[rows], f_send.at[4], f_recv.at[4], partner)
    c4.start()
    c4.wait()
    out[:FEAT + CLS, :] = fin[:FEAT + CLS, :]
    out[FEAT + CLS:, :] = fin[FEAT + CLS:, :] / count


def solution(mesh):
    vmem, anywhere = pl.BlockSpec(memory_space=pltpu.VMEM), pl.BlockSpec(memory_space=pl.ANY)

    def local_step(adj, feat, w_one, w_two, label, mask):
        feat_t = jnp.pad(feat.T, ((0, FEAT - 100), (0, 0)))
        w1t = jnp.pad(w_one.astype(BF16).T, ((0, 0), (0, FEAT - 100)))
        w2 = jnp.pad(w_two.astype(BF16), ((0, 0), (0, 1)))
        mask_row = mask.astype(F32).reshape(1, ROWS)
        out = pl.pallas_call(
            kernel,
            out_shape=jax.ShapeDtypeStruct((RED, HID), F32),
            in_specs=[anywhere, anywhere, vmem, vmem, vmem, vmem, vmem, anywhere],
            out_specs=vmem,
            scratch_shapes=[
                pltpu.VMEM((SLOTS, ROWS, TILE), BF16),
                pltpu.VMEM((16, FEAT, TILE), BF16),
                pltpu.VMEM((16, FEAT, TILE), BF16),
                pltpu.VMEM((FEAT, ROWS), F32),
                pltpu.VMEM((HID, ROWS), F32),
                pltpu.VMEM((HID, TILE), BF16),
                pltpu.VMEM((HID, ROWS), BF16),
                pltpu.VMEM((HID, ROWS), BF16),
                pltpu.VMEM((8, 1, ROWS), F32),
                pltpu.VMEM((CLS, ROWS), BF16),
                pltpu.VMEM((8, HID, TILE), F32),
                pltpu.VMEM((8, HID, TILE), F32),
                pltpu.VMEM((8, HID, TILE), F32),
                pltpu.VMEM((6, HID, TILE), F32),
                pltpu.VMEM((RED, HID), F32),
                pltpu.VMEM((RED, HID), F32),
                pltpu.VMEM((4, RED // 2, HID), F32),
                pltpu.VMEM((RED, HID), F32),
                pltpu.SemaphoreType.DMA((SLOTS,)),
                pltpu.SemaphoreType.DMA((3,)),
                pltpu.SemaphoreType.DMA((2, 16)),
                pltpu.SemaphoreType.DMA((2, 16)),
                pltpu.SemaphoreType.DMA((8,)),
                pltpu.SemaphoreType.DMA((8,)),
                pltpu.SemaphoreType.DMA((8,)),
                pltpu.SemaphoreType.DMA((8,)),
                pltpu.SemaphoreType.DMA((6,)),
                pltpu.SemaphoreType.DMA((6,)),
                pltpu.SemaphoreType.DMA((5,)),
                pltpu.SemaphoreType.DMA((5,)),
            ],
            compiler_params=pltpu.CompilerParams(collective_id=0, has_side_effects=True, vmem_limit_bytes=67043328),
            name='gcn_step',
        )(adj, feat_t, w1t, w2.T, w2, label.reshape(1, ROWS), mask_row, mask_row)
        return (out[FEAT + CLS, :1], out[:100], out[FEAT:FEAT + 47].T)

    return jax.shard_map(local_step, mesh=mesh, in_specs=(P('nodes', None), P('nodes', None), P(None, None), P(None, None), P('nodes'), P('nodes')), out_specs=(P(None), P(None, None), P(None, None)), check_vma=False)
```

```python
import jax
import jax.numpy as jnp
from jax import lax
from jax.experimental import pallas as pl
from jax.experimental.pallas import tpu as pltpu
from jax.sharding import PartitionSpec as P

MESH = pl.DeviceIdType.MESH
F32, BF16 = jnp.float32, jnp.bfloat16
LANE_CONTRACT = (((1,), (1,)), ((), ()))

ROWS = 2048
TILE = 1024
SLOTS = 8
FEAT = 104
HID = 128
CLS = 48
RED = FEAT + CLS + 8


def kernel(adj, feat, w_one, w_two_t, label, mask, mask_any, out,
           w1t, w2t, w2, ring, xbuf, sbuf, acc1, acc2, hid, s2t, ut, mall, dcls,
           pbuf, rbuf, cbuf, rsbuf, red, redp, half, fin,
           ring_sem, loc_sem, ag_send, ag_recv, m_send, m_recv,
           d_send, d_recv, rs_send, rs_recv, f_send, f_recv):
    me = lax.axis_index('nodes')
    core, px, py = me % 2, (me // 2) % 2, me // 4

    def device(fy, fx, fc):
        return 4 * ((py + fy) % 2) + 2 * ((px + fx) % 2) + (core + fc) % 2

    partner, xn, yn, diag = device(0, 0, 1), device(0, 1, 0), device(1, 0, 0), device(1, 1, 0)

    def columns(u):
        s, back = u % 16, u // 32
        g = (1 - back) * (s // 4) + back * (3 - s // 4)
        r = (1 - back) * (s % 2) + back * ((s // 2) % 2)
        fc = (1 - back) * ((s // 2) % 2) + back * (1 - s % 2)
        t = (g + 1) // 2
        fx, fy = (t + 1 - r) // 2, (t + r) // 2
        h = (r + (g // 2) * (3 - g)) % 2
        return pl.multiple_of(device(fy, fx, fc) * ROWS + h * TILE, TILE)

    def tile(u):
        slot = u % SLOTS
        return pltpu.make_async_copy(adj.at[:, pl.ds(columns(u), TILE)], ring.at[slot], ring_sem.at[slot])

    def remote(src, dst, ssem, rsem, dev):
        return pltpu.make_async_remote_copy(src_ref=src, dst_ref=dst, send_sem=ssem, recv_sem=rsem,
                                            device_id=(dev,), device_id_type=MESH)

    for u in range(SLOTS):
        tile(u).start()
    own = [pltpu.make_async_copy(feat.at[:, pl.ds(h * TILE, TILE)], xbuf.at[h], loc_sem.at[h]) for h in range(2)]
    own.append(pltpu.make_async_copy(mask_any, mall.at[0], loc_sem.at[2]))
    for c in own:
        c.start()

    w1t[...] = jnp.concatenate([w_one[...], jnp.zeros((28, HID), F32)], 0).T[:, :FEAT].astype(BF16)
    wide = jnp.concatenate([w_two_t[...], jnp.zeros((81, HID), F32)], 0)
    w2t[...] = wide[:CLS].astype(BF16)
    w2[...] = wide.T[:, :CLS].astype(BF16)
    acc1[...] = jnp.zeros_like(acc1)
    acc2[...] = jnp.zeros_like(acc2)

    peers = [device(e // 4, (e // 2) % 2, e % 2) for e in range(8)]
    barrier = pltpu.get_barrier_semaphore()
    for e in range(1, 8):
        pl.semaphore_signal(barrier, inc=1, device_id=(peers[e],), device_id_type=MESH)
    with jax.named_scope('barrier'):
        pl.semaphore_wait(barrier, 7)

    def gather_copy(ph, buf, src, step, dev):
        return remote(src, buf.at[step], ag_send.at[ph, step], ag_recv.at[ph, step], dev)

    def gather_start(ph, buf, srcs):
        for step, h, dev in ((4, 0, xn), (5, 1, yn), (2, 0, partner), (3, 1, partner), (8, 1, xn), (9, 0, yn)):
            gather_copy(ph, buf, srcs[h], step, dev).start()

    def gather_step(ph, buf, s):
        @pl.when(s >= 2)
        def _():
            gather_copy(ph, buf, buf.at[s], s, partner).wait_recv()

        @pl.when((s >= 4) & (s % 4 < 2))
        def _():
            gather_copy(ph, buf, buf.at[s], s + 2, partner).start()

        @pl.when(s == 4)
        def _():
            gather_copy(ph, buf, buf.at[s], 12, yn).start()

        @pl.when(s == 5)
        def _():
            gather_copy(ph, buf, buf.at[s], 13, xn).start()

    def gather_finish(ph, buf):
        for step in range(2, 16):
            gather_copy(ph, buf, buf.at[0], step, partner).wait_send()

    gather_start(0, xbuf, [feat.at[:, pl.ds(h * TILE, TILE)] for h in range(2)])
    m_copies = [remote(mask_any, mall.at[e], m_send.at[e], m_recv.at[e], peers[e]) for e in range(1, 8)]
    for c in m_copies:
        c.start()
    for c in own:
        c.wait()


    def first(s, _):
        with jax.named_scope('wait1'):
            tile(s).wait()
            gather_step(0, xbuf, s)
        acc1[:100, :] += lax.dot_general(xbuf[s], ring[s % SLOTS], LANE_CONTRACT, preferred_element_type=F32)
        tile(s + SLOTS).start()
        return 0

    with jax.named_scope('pass1'):
        lax.fori_loop(0, 16, first, 0)
    for h in range(2):
        sbuf[h] = acc1[:, h * TILE:(h + 1) * TILE].astype(BF16)
    gather_start(1, sbuf, [sbuf.at[h] for h in range(2)])


    def second(s, _):
        with jax.named_scope('wait2'):
            tile(s + 16).wait()
            gather_step(1, sbuf, s)
        hid[...] = jnp.maximum(jnp.dot(w1t[...], sbuf[s], preferred_element_type=F32), 0.0).astype(BF16)
        acc2[...] += lax.dot_general(hid[...], ring[s % SLOTS], LANE_CONTRACT, preferred_element_type=F32)
        tile(s + 16 + SLOTS).start()
        return 0

    with jax.named_scope('pass2'):
        lax.fori_loop(0, 16, second, 0)

    with jax.named_scope('wait_m'):
        for c in m_copies:
            c.wait()
    count = jnp.sum(jnp.sum(mall[...], axis=0).astype(F32))
    classes = lax.broadcasted_iota(jnp.int32, (CLS, 512), 0)

    def heads(i, loss):
        cols = pl.ds(pl.multiple_of(i * 512, 512), 512)
        agg = acc2[:, cols].astype(BF16)
        s2t[:, cols] = agg
        z = jnp.dot(w2t[...], agg, preferred_element_type=F32)
        z = jnp.where(classes < 47, z, -1e30)
        z = z - jnp.max(z, axis=0, keepdims=True)
        logp = z - jnp.log(jnp.sum(jnp.exp(z), axis=0, keepdims=True))
        onehot = (label[:, cols] == classes).astype(F32)
        weight = mask[:, cols].astype(F32)
        g2 = (weight * (jnp.exp(logp) - onehot) / count).astype(BF16)
        dcls[:, cols] = g2
        ut[:, cols] = jnp.dot(w2[...], g2, preferred_element_type=F32).astype(BF16)
        return loss + weight * jnp.sum(jnp.where(label[:, cols] == classes, logp, 0.0), axis=0, keepdims=True)

    loss = lax.fori_loop(0, ROWS // 512, heads, jnp.zeros((1, 512), F32))

    to_y = (True, False, False, True, False, True)

    def pair_copy(j):
        return remote(pbuf.at[j], rbuf.at[j], d_send.at[j], d_recv.at[j], partner)

    def link_copy(j):
        return remote(cbuf.at[j], rsbuf.at[j], rs_send.at[j], rs_recv.at[j], yn if to_y[j] else xn)

    def finalize(j):
        with jax.named_scope('wait_pair'):
            pair_copy(j).wait_recv()
        if j in (4, 5):
            with jax.named_scope('wait_link'):
                link_copy(j - 4).wait_recv()
            cbuf[j] = (cbuf[j] + rbuf[j]) + rsbuf[j - 4]
        else:
            cbuf[j] = cbuf[j] + rbuf[j]
        if j < 6:
            link_copy(j).start()

    def third(j, _):
        u = 32 + 2 * j
        tile(u).wait()
        pbuf[j] = jnp.dot(ut[...], ring[u % SLOTS], preferred_element_type=F32)
        pair_copy(j).start()

        @pl.when(j < 4)
        def _():
            tile(u + SLOTS).start()

        tile(u + 1).wait()
        cbuf[j] = jnp.dot(ut[...], ring[(u + 1) % SLOTS], preferred_element_type=F32)

        @pl.when(j < 4)
        def _():
            tile(u + 1 + SLOTS).start()

        for jj in range(7):
            @pl.when(j == jj + 1)
            def _(jj=jj):
                finalize(jj)
        return 0

    with jax.named_scope('pass3'):
        lax.fori_loop(0, 8, third, 0)
    finalize(7)

    red[FEAT:FEAT + CLS, :] = lax.dot_general(dcls[...], s2t[...], LANE_CONTRACT, preferred_element_type=F32)
    red[FEAT + CLS:, :] = jnp.broadcast_to(-jnp.sum(loss), (8, HID))
    gather_finish(0, xbuf)
    gather_finish(1, sbuf)
    for j in range(8):
        pair_copy(j).wait_send()

    dw1 = jnp.zeros((FEAT, HID), F32)
    for h, (a, b) in enumerate(((3, 4), (2, 5))):
        z1 = jnp.dot(w1t[...], sbuf[h], preferred_element_type=F32)
        with jax.named_scope('wait_own'):
            link_copy(a).wait_recv()
            link_copy(b).wait_recv()
        g1 = jnp.where(z1 > 0.0, (cbuf[6 + h] + rsbuf[a]) + rsbuf[b], 0.0).astype(BF16)
        dw1 = dw1 + lax.dot_general(sbuf[h], g1, LANE_CONTRACT, preferred_element_type=F32)
    red[:FEAT, :] = dw1
    for j in range(6):
        link_copy(j).wait_send()

    c0 = remote(red, redp, f_send.at[0], f_recv.at[0], partner)
    with jax.named_scope('sum_chip'):
        c0.start()
        c0.wait()
    rows = pl.ds(pl.multiple_of(core * (RED // 2), 8), RED // 2)
    half[0] = red[rows, :] + redp[rows, :]
    copies = [remote(half.at[0], half.at[e], f_send.at[e], f_recv.at[e], dev) for e, dev in ((1, xn), (2, yn), (3, diag))]
    with jax.named_scope('sum_chips'):
        for c in copies:
            c.start()
        for c in copies:
            c.wait()
    fin[rows, :] = (half[0] + half[1]) + (half[2] + half[3])
    c4 = remote(fin.at[rows], fin.at[rows], f_send.at[4], f_recv.at[4], partner)
    with jax.named_scope('sum_pair'):
        c4.start()
        c4.wait()
    out[:FEAT + CLS, :] = fin[:FEAT + CLS, :]
    out[FEAT + CLS:, :] = fin[FEAT + CLS:, :] / count


def split(total, loss, dw_one, dw_two_t):
    loss[...] = total[FEAT + CLS:FEAT + CLS + 1, :1]
    dw_one[...] = total[:100, :]
    dw_two_t[...] = total[FEAT:FEAT + 47, :]


def solution(mesh):
    vmem, anywhere = pl.BlockSpec(memory_space=pltpu.VMEM), pl.BlockSpec(memory_space=pl.ANY)

    def local_step(adj, feat, w_one, w_two, label, mask):
        mask_row = mask.reshape(1, ROWS)
        out = pl.pallas_call(
            kernel,
            out_shape=jax.ShapeDtypeStruct((RED, HID), F32),
            in_specs=[anywhere, anywhere, vmem, vmem, vmem, vmem, anywhere],
            out_specs=vmem,
            scratch_shapes=[
                pltpu.VMEM((HID, FEAT), BF16),
                pltpu.VMEM((CLS, HID), BF16),
                pltpu.VMEM((HID, CLS), BF16),
                pltpu.VMEM((SLOTS, ROWS, TILE), BF16),
                pltpu.VMEM((16, 100, TILE), BF16),
                pltpu.VMEM((16, FEAT, TILE), BF16),
                pltpu.VMEM((FEAT, ROWS), F32),
                pltpu.VMEM((HID, ROWS), F32),
                pltpu.VMEM((HID, TILE), BF16),
                pltpu.VMEM((HID, ROWS), BF16),
                pltpu.VMEM((HID, ROWS), BF16),
                pltpu.VMEM((8, 1, ROWS), jnp.int32),
                pltpu.VMEM((CLS, ROWS), BF16),
                pltpu.VMEM((8, HID, TILE), F32),
                pltpu.VMEM((8, HID, TILE), F32),
                pltpu.VMEM((8, HID, TILE), F32),
                pltpu.VMEM((6, HID, TILE), F32),
                pltpu.VMEM((RED, HID), F32),
                pltpu.VMEM((RED, HID), F32),
                pltpu.VMEM((4, RED // 2, HID), F32),
                pltpu.VMEM((RED, HID), F32),
                pltpu.SemaphoreType.DMA((SLOTS,)),
                pltpu.SemaphoreType.DMA((3,)),
                pltpu.SemaphoreType.DMA((2, 16)),
                pltpu.SemaphoreType.DMA((2, 16)),
                pltpu.SemaphoreType.DMA((8,)),
                pltpu.SemaphoreType.DMA((8,)),
                pltpu.SemaphoreType.DMA((8,)),
                pltpu.SemaphoreType.DMA((8,)),
                pltpu.SemaphoreType.DMA((6,)),
                pltpu.SemaphoreType.DMA((6,)),
                pltpu.SemaphoreType.DMA((5,)),
                pltpu.SemaphoreType.DMA((5,)),
            ],
            compiler_params=pltpu.CompilerParams(collective_id=0, has_side_effects=True, vmem_limit_bytes=67043328),
            name='gcn_step',
        )(adj, feat.T, w_one, w_two.T, label.reshape(1, ROWS), mask_row, mask_row)
        loss, dw_one, dw_two_t = pl.pallas_call(
            split,
            out_shape=[jax.ShapeDtypeStruct(shape, F32) for shape in ((1, 1), (100, HID), (47, HID))],
            in_specs=[vmem],
            out_specs=[vmem] * 3,
            name='split',
        )(out)
        return (loss.reshape(1), dw_one, dw_two_t.T)

    return jax.shard_map(local_step, mesh=mesh, in_specs=(P('nodes', None), P('nodes', None), P(None, None), P(None, None), P('nodes'), P('nodes')), out_specs=(P(None), P(None, None), P(None, None)), check_vma=False)
```

```python
import functools

import jax
import jax.numpy as jnp
from jax import lax
from jax.experimental import pallas as pl
from jax.experimental.pallas import tpu as pltpu
from jax.sharding import PartitionSpec as P

MESH = pl.DeviceIdType.MESH
F32, BF16 = jnp.float32, jnp.bfloat16
LANE_CONTRACT = (((1,), (1,)), ((), ()))

ROWS = 2048
TILE = 1024
SLOTS = 8
FLIP = 1280
FEAT = 104
HID = 128
CLS = 48
RED = FEAT + CLS + 8


def kernel(adj, feat, w_one, w_two_t, label, mask, mask_any, out,
           w1t, w2t, w2, ring, flip, xbuf, sbuf, acc1, acc2, hid, s2t, mall, dcls,
           pbuf, rbuf, cbuf, rsbuf, red, redp, half, fin,
           ring_sem, loc_sem, ag_send, ag_recv, m_send, m_recv,
           d_send, d_recv, rs_send, rs_recv, f_send, f_recv):
    me = lax.axis_index('nodes')
    core, px, py = me % 2, (me // 2) % 2, me // 4

    def device(fy, fx, fc):
        return 4 * ((py + fy) % 2) + 2 * ((px + fx) % 2) + (core + fc) % 2

    partner, xn, yn, diag = device(0, 0, 1), device(0, 1, 0), device(1, 0, 0), device(1, 1, 0)

    def columns(u):
        s, back = u % 16, u // 32
        g, r = (1 - back) * (s // 4) + back * (3 - s // 4), s % 2
        fc = (back + (s // 2) % 2) % 2
        t = (g + 1) // 2
        fx, fy = (t + 1 - r) // 2, (t + r) // 2
        h = (r + (g // 2) * (3 - g)) % 2
        return pl.multiple_of(device(fy, fx, fc) * ROWS + h * TILE, TILE)

    def tile(u):
        slot = u % SLOTS
        return pltpu.make_async_copy(adj.at[:, pl.ds(columns(u), TILE)], ring.at[slot], ring_sem.at[slot])

    def remote(src, dst, ssem, rsem, dev):
        return pltpu.make_async_remote_copy(src_ref=src, dst_ref=dst, send_sem=ssem, recv_sem=rsem,
                                            device_id=(dev,), device_id_type=MESH)

    own = [pltpu.make_async_copy(feat.at[:, pl.ds(h * TILE, TILE)], xbuf.at[h], loc_sem.at[h]) for h in range(2)]
    own.append(pltpu.make_async_copy(mask_any, mall.at[0], loc_sem.at[2]))
    for c in own:
        c.start()
    for u in range(SLOTS):
        tile(u).start()
    w1t[...] = jnp.concatenate([w_one[...], jnp.zeros((28, HID), F32)], 0).T[:, :FEAT].astype(BF16)
    wide = jnp.concatenate([w_two_t[...], jnp.zeros((81, HID), F32)], 0)
    w2t[...] = wide[:CLS].astype(BF16)
    w2[...] = wide.T[:, :CLS].astype(BF16)
    acc1[...] = jnp.zeros_like(acc1)
    acc2[...] = jnp.zeros_like(acc2)

    peers = [device(e // 4, (e // 2) % 2, e % 2) for e in range(8)]
    barrier = pltpu.get_barrier_semaphore()
    for e in range(1, 8):
        pl.semaphore_signal(barrier, inc=1, device_id=(peers[e],), device_id_type=MESH)
    with jax.named_scope('barrier'):
        pl.semaphore_wait(barrier, 7)

    def gather_copy(ph, buf, src, step, dev):
        return remote(src, buf.at[step], ag_send.at[ph, step], ag_recv.at[ph, step], dev)

    def gather_start(ph, buf, srcs):
        for step, h, dev in ((4, 0, xn), (5, 1, yn), (2, 0, partner), (3, 1, partner), (8, 1, xn), (9, 0, yn)):
            gather_copy(ph, buf, srcs[h], step, dev).start()

    def gather_step(ph, buf, s):
        @pl.when(s >= 2)
        def _():
            gather_copy(ph, buf, buf.at[s], s, partner).wait_recv()

        @pl.when((s >= 4) & (s % 4 < 2))
        def _():
            gather_copy(ph, buf, buf.at[s], s + 2, partner).start()

        @pl.when(s == 4)
        def _():
            gather_copy(ph, buf, buf.at[s], 12, yn).start()

        @pl.when(s == 5)
        def _():
            gather_copy(ph, buf, buf.at[s], 13, xn).start()

    def gather_finish(ph, buf):
        for step in range(2, 16):
            gather_copy(ph, buf, buf.at[0], step, partner).wait_send()

    gather_start(0, xbuf, [feat.at[:, pl.ds(h * TILE, TILE)] for h in range(2)])
    m_copies = [remote(mask_any, mall.at[e], m_send.at[e], m_recv.at[e], peers[e]) for e in range(1, 8)]
    for c in m_copies:
        c.start()
    for c in own:
        c.wait()

    def flip_rows(u):
        return ring[u % SLOTS, :FLIP, :].T

    def pair(acc, rows, x, u):
        for k in range(2):
            flip[1 - k] = flip_rows(u + k + 1)
            acc[:rows, FLIP:] += lax.dot_general(x(k), ring[(u + k) % SLOTS, FLIP:, :], LANE_CONTRACT, preferred_element_type=F32)
            acc[:rows, :FLIP] += jnp.dot(x(k), flip[k], preferred_element_type=F32)

    tile(0).wait()
    flip[0] = flip_rows(0)

    def first(i, _):
        s = 2 * i
        with jax.named_scope('wait1'):
            for k in range(2):
                tile(s + k + 1).wait()
                gather_step(0, xbuf, s + k)
        pair(acc1, 100, lambda k: xbuf[s + k], s)
        for k in range(2):
            tile(s + k + SLOTS).start()
        return 0

    with jax.named_scope('pass1'):
        lax.fori_loop(0, 8, first, 0)
    for h in range(2):
        sbuf[h] = acc1[:, h * TILE:(h + 1) * TILE].astype(BF16)
    gather_start(1, sbuf, [sbuf.at[h] for h in range(2)])

    def second(i, _):
        s = 2 * i
        with jax.named_scope('wait2'):
            for k in range(2):
                tile(s + k + 17).wait()
                gather_step(1, sbuf, s + k)
        for k in range(2):
            hid[:, k * TILE:(k + 1) * TILE] = jnp.maximum(jnp.dot(w1t[...], sbuf[s + k], preferred_element_type=F32), 0.0).astype(BF16)
        pair(acc2, HID, lambda k: hid[:, k * TILE:(k + 1) * TILE], s + 16)
        for k in range(2):
            tile(s + k + 16 + SLOTS).start()
        return 0

    with jax.named_scope('pass2'):
        lax.fori_loop(0, 8, second, 0)

    ut = hid
    with jax.named_scope('wait_m'):
        for c in m_copies:
            c.wait()
    count = jnp.sum(jnp.sum(mall[...], axis=0).astype(F32))
    classes = lax.broadcasted_iota(jnp.int32, (CLS, 512), 0)

    def heads(i, loss):
        cols = pl.ds(pl.multiple_of(i * 512, 512), 512)
        agg = acc2[:, cols].astype(BF16)
        s2t[:, cols] = agg
        z = jnp.dot(w2t[...], agg, preferred_element_type=F32)
        z = jnp.where(classes < 47, z, -1e30)
        z = z - jnp.max(z, axis=0, keepdims=True)
        logp = z - jnp.log(jnp.sum(jnp.exp(z), axis=0, keepdims=True))
        onehot = (label[:, cols] == classes).astype(F32)
        weight = mask[:, cols].astype(F32)
        g2 = (weight * (jnp.exp(logp) - onehot) / count).astype(BF16)
        dcls[:, cols] = g2
        ut[:, cols] = jnp.dot(w2[...], g2, preferred_element_type=F32).astype(BF16)
        return loss + weight * jnp.sum(jnp.where(label[:, cols] == classes, logp, 0.0), axis=0, keepdims=True)

    loss = lax.fori_loop(0, ROWS // 512, heads, jnp.zeros((1, 512), F32))

    to_y = (True, False, False, True, False, True)

    def pair_copy(j):
        return remote(pbuf.at[j % 4], rbuf.at[j], d_send.at[j], d_recv.at[j], partner)

    def link_copy(j):
        return remote(cbuf.at[j], rsbuf.at[j], rs_send.at[j], rs_recv.at[j], yn if to_y[j] else xn)

    def finalize(j):
        with jax.named_scope('wait_pair'):
            pair_copy(j).wait_recv()
        if j in (4, 5):
            with jax.named_scope('wait_link'):
                link_copy(j - 4).wait_recv()
            cbuf[j] = (cbuf[j] + rbuf[j]) + rsbuf[j - 4]
        else:
            cbuf[j] = cbuf[j] + rbuf[j]
        if j < 6:
            link_copy(j).start()

    def third(k, _):
        for q in range(4):
            u, j = 32 + 4 * k + q, 2 * k + q % 2
            if q == 0:
                pl.when(k > 0)(tile(u).wait)
            else:
                tile(u).wait()
            term = jnp.dot(ut[...], ring[u % SLOTS], preferred_element_type=F32)
            if q < 2:
                pl.when(k >= 2)(pair_copy(j - 4).wait_send)
                pbuf[j % 4] = term
                pair_copy(j).start()
            else:
                cbuf[j] = term
            pl.when(k < 2)(tile(u + SLOTS).start)
            if q >= 2:
                for kk in range(4):
                    pl.when(k == kk)(functools.partial(finalize, 2 * kk + q - 2))
        return 0

    with jax.named_scope('pass3'):
        lax.fori_loop(0, 4, third, 0)

    red[FEAT:FEAT + CLS, :] = lax.dot_general(dcls[...], s2t[...], LANE_CONTRACT, preferred_element_type=F32)
    red[FEAT + CLS:, :] = jnp.broadcast_to(-jnp.sum(loss), (8, HID))
    gather_finish(0, xbuf)
    gather_finish(1, sbuf)
    for j in range(4, 8):
        pair_copy(j).wait_send()

    dw1 = jnp.zeros((FEAT, HID), F32)
    for h, (a, b) in enumerate(((3, 4), (2, 5))):
        z1 = jnp.dot(w1t[...], sbuf[h], preferred_element_type=F32)
        with jax.named_scope('wait_own'):
            link_copy(a).wait_recv()
            link_copy(b).wait_recv()
        g1 = jnp.where(z1 > 0.0, (cbuf[6 + h] + rsbuf[a]) + rsbuf[b], 0.0).astype(BF16)
        dw1 = dw1 + lax.dot_general(sbuf[h], g1, LANE_CONTRACT, preferred_element_type=F32)
    red[:FEAT, :] = dw1
    for j in range(6):
        link_copy(j).wait_send()

    c0 = remote(red, redp, f_send.at[0], f_recv.at[0], partner)
    with jax.named_scope('sum_chip'):
        c0.start()
        c0.wait()
    rows = pl.ds(pl.multiple_of(core * (RED // 2), 8), RED // 2)
    half[0] = red[rows, :] + redp[rows, :]
    copies = [remote(half.at[0], half.at[e], f_send.at[e], f_recv.at[e], dev) for e, dev in ((1, xn), (2, yn), (3, diag))]
    with jax.named_scope('sum_chips'):
        for c in copies:
            c.start()
        for c in copies:
            c.wait()
    fin[rows, :] = (half[0] + half[1]) + (half[2] + half[3])
    c4 = remote(fin.at[rows], fin.at[rows], f_send.at[4], f_recv.at[4], partner)
    with jax.named_scope('sum_pair'):
        c4.start()
        c4.wait()
    out[:FEAT + CLS, :] = fin[:FEAT + CLS, :]
    out[FEAT + CLS:, :] = fin[FEAT + CLS:, :] / count


def split(total, loss, dw_one, dw_two_t):
    loss[...] = total[FEAT + CLS:FEAT + CLS + 1, :1]
    dw_one[...] = total[:100, :]
    dw_two_t[...] = total[FEAT:FEAT + 47, :]


def solution(mesh):
    vmem, anywhere = pl.BlockSpec(memory_space=pltpu.VMEM), pl.BlockSpec(memory_space=pl.ANY)

    def local_step(adj, feat, w_one, w_two, label, mask):
        mask_row = mask.reshape(1, ROWS)
        out = pl.pallas_call(
            kernel,
            out_shape=jax.ShapeDtypeStruct((RED, HID), F32),
            in_specs=[anywhere, anywhere, vmem, vmem, vmem, vmem, anywhere],
            out_specs=vmem,
            scratch_shapes=[
                pltpu.VMEM((HID, FEAT), BF16),
                pltpu.VMEM((CLS, HID), BF16),
                pltpu.VMEM((HID, CLS), BF16),
                pltpu.VMEM((SLOTS, ROWS, TILE), BF16),
                pltpu.VMEM((2, TILE, FLIP), BF16),
                pltpu.VMEM((16, 100, TILE), BF16),
                pltpu.VMEM((16, FEAT, TILE), BF16),
                pltpu.VMEM((FEAT, ROWS), F32),
                pltpu.VMEM((HID, ROWS), F32),
                pltpu.VMEM((HID, ROWS), BF16),
                pltpu.VMEM((HID, ROWS), BF16),
                pltpu.VMEM((8, 1, ROWS), jnp.int32),
                pltpu.VMEM((CLS, ROWS), BF16),
                pltpu.VMEM((4, HID, TILE), F32),
                pltpu.VMEM((8, HID, TILE), F32),
                pltpu.VMEM((8, HID, TILE), F32),
                pltpu.VMEM((6, HID, TILE), F32),
                pltpu.VMEM((RED, HID), F32),
                pltpu.VMEM((RED, HID), F32),
                pltpu.VMEM((4, RED // 2, HID), F32),
                pltpu.VMEM((RED, HID), F32),
                pltpu.SemaphoreType.DMA((SLOTS,)),
                pltpu.SemaphoreType.DMA((3,)),
                pltpu.SemaphoreType.DMA((2, 16)),
                pltpu.SemaphoreType.DMA((2, 16)),
                pltpu.SemaphoreType.DMA((8,)),
                pltpu.SemaphoreType.DMA((8,)),
                pltpu.SemaphoreType.DMA((8,)),
                pltpu.SemaphoreType.DMA((8,)),
                pltpu.SemaphoreType.DMA((6,)),
                pltpu.SemaphoreType.DMA((6,)),
                pltpu.SemaphoreType.DMA((5,)),
                pltpu.SemaphoreType.DMA((5,)),
            ],
            compiler_params=pltpu.CompilerParams(collective_id=0, has_side_effects=True, vmem_limit_bytes=67043328),
            name='gcn_step',
        )(adj, feat.T, w_one, w_two.T, label.reshape(1, ROWS), mask_row, mask_row)
        loss, dw_one, dw_two_t = pl.pallas_call(
            split,
            out_shape=[jax.ShapeDtypeStruct(shape, F32) for shape in ((1, 1), (100, HID), (47, HID))],
            in_specs=[vmem],
            out_specs=[vmem] * 3,
            name='split',
        )(out)
        return (loss.reshape(1), dw_one, dw_two_t.T)

    return jax.shard_map(local_step, mesh=mesh, in_specs=(P('nodes', None), P('nodes', None), P(None, None), P(None, None), P('nodes'), P('nodes')), out_specs=(P(None), P(None, None), P(None, None)), check_vma=False)
```

```python
import functools

import jax
import jax.numpy as jnp
from jax import lax
from jax.experimental import pallas as pl
from jax.experimental.pallas import tpu as pltpu
from jax.sharding import PartitionSpec as P

MESH = pl.DeviceIdType.MESH
F32, BF16 = jnp.float32, jnp.bfloat16
LANE_CONTRACT = (((1,), (1,)), ((), ()))

ROWS = 2048
TILE = 1024
SLOTS = 8
FLIP = 1280
FEAT = 104
HID = 128
CLS = 48
RED1, RED2 = 112, 64
SUB = TILE // 2


def kernel(adj, feat, w_one, w_two_t, label, mask, mask_any, out,
           w1t, w2t, w2, ring, flip, xbuf, sbuf, acc1, acc2, hid, s2t, mall, dcls,
           pbuf, rbuf, cbuf, rsbuf, red1, redp1, half1, red2, redp2, half2, fin,
           ring_sem, loc_sem, ag_send, ag_recv, m_send, m_recv,
           d_send, d_recv, rs_send, rs_recv, f_send, f_recv):
    me = lax.axis_index('nodes')
    core, px, py = me % 2, (me // 2) % 2, me // 4

    def device(fy, fx, fc):
        return 4 * ((py + fy) % 2) + 2 * ((px + fx) % 2) + (core + fc) % 2

    partner, xn, yn, diag = device(0, 0, 1), device(0, 1, 0), device(1, 0, 0), device(1, 1, 0)

    def columns(u):
        s, back = u % 16, u // 32
        g, r = (1 - back) * (s // 4) + back * (3 - s // 4), s % 2
        fc = (back + (s // 2) % 2) % 2
        t = (g + 1) // 2
        fx, fy = (t + 1 - r) // 2, (t + r) // 2
        h = (r + (g // 2) * (3 - g)) % 2
        return pl.multiple_of(device(fy, fx, fc) * ROWS + h * TILE, TILE)

    def tile(u):
        slot = u % SLOTS
        return pltpu.make_async_copy(adj.at[:, pl.ds(columns(u), TILE)], ring.at[slot], ring_sem.at[slot])

    def remote(src, dst, ssem, rsem, dev):
        return pltpu.make_async_remote_copy(src_ref=src, dst_ref=dst, send_sem=ssem, recv_sem=rsem,
                                            device_id=(dev,), device_id_type=MESH)

    own = [pltpu.make_async_copy(feat.at[:, pl.ds(h * TILE, TILE)], xbuf.at[h], loc_sem.at[h]) for h in range(2)]
    own.append(pltpu.make_async_copy(mask_any, mall.at[0], loc_sem.at[2]))
    for c in own:
        c.start()
    for u in range(SLOTS):
        tile(u).start()
    w1t[...] = jnp.concatenate([w_one[...], jnp.zeros((28, HID), F32)], 0).T[:, :FEAT].astype(BF16)
    wide = jnp.concatenate([w_two_t[...], jnp.zeros((81, HID), F32)], 0)
    w2t[...] = wide[:CLS].astype(BF16)
    w2[...] = wide.T[:, :CLS].astype(BF16)
    acc1[...] = jnp.zeros_like(acc1)
    acc2[...] = jnp.zeros_like(acc2)

    peers = [device(e // 4, (e // 2) % 2, e % 2) for e in range(8)]
    barrier = pltpu.get_barrier_semaphore()
    for e in range(1, 8):
        pl.semaphore_signal(barrier, inc=1, device_id=(peers[e],), device_id_type=MESH)
    with jax.named_scope('barrier'):
        pl.semaphore_wait(barrier, 7)

    def gather_copy(ph, buf, src, step, dev):
        return remote(src, buf.at[step], ag_send.at[ph, step], ag_recv.at[ph, step], dev)

    def gather_start(ph, buf, srcs):
        for step, h, dev in ((4, 0, xn), (5, 1, yn), (2, 0, partner), (3, 1, partner), (8, 1, xn), (9, 0, yn)):
            gather_copy(ph, buf, srcs[h], step, dev).start()

    def gather_step(ph, buf, s):
        @pl.when(s >= 2)
        def _():
            gather_copy(ph, buf, buf.at[s], s, partner).wait_recv()

        @pl.when((s >= 4) & (s % 4 < 2))
        def _():
            gather_copy(ph, buf, buf.at[s], s + 2, partner).start()

        @pl.when(s == 4)
        def _():
            gather_copy(ph, buf, buf.at[s], 12, yn).start()

        @pl.when(s == 5)
        def _():
            gather_copy(ph, buf, buf.at[s], 13, xn).start()

    def gather_finish(ph, buf):
        for step in range(2, 16):
            gather_copy(ph, buf, buf.at[0], step, partner).wait_send()

    gather_start(0, xbuf, [feat.at[:, pl.ds(h * TILE, TILE)] for h in range(2)])
    m_copies = [remote(mask_any, mall.at[e], m_send.at[e], m_recv.at[e], peers[e]) for e in range(1, 8)]
    for c in m_copies:
        c.start()
    for c in own:
        c.wait()

    def flip_rows(u):
        return ring[u % SLOTS, :FLIP, :].T

    def pair(acc, rows, x, u):
        for k in range(2):
            flip[1 - k] = flip_rows(u + k + 1)
            acc[:rows, FLIP:] += lax.dot_general(x(k), ring[(u + k) % SLOTS, FLIP:, :], LANE_CONTRACT, preferred_element_type=F32)
            acc[:rows, :FLIP] += jnp.dot(x(k), flip[k], preferred_element_type=F32)

    tile(0).wait()
    flip[0] = flip_rows(0)

    def first(i, _):
        s = 2 * i
        with jax.named_scope('wait1'):
            for k in range(2):
                tile(s + k + 1).wait()
                gather_step(0, xbuf, s + k)
        pair(acc1, 100, lambda k: xbuf[s + k], s)
        for k in range(2):
            tile(s + k + SLOTS).start()
        return 0

    with jax.named_scope('pass1'):
        lax.fori_loop(0, 8, first, 0)
    for h in range(2):
        sbuf[h] = acc1[:, h * TILE:(h + 1) * TILE].astype(BF16)
    gather_start(1, sbuf, [sbuf.at[h] for h in range(2)])

    def second(i, _):
        s = 2 * i
        with jax.named_scope('wait2'):
            for k in range(2):
                tile(s + k + 17).wait()
                gather_step(1, sbuf, s + k)
        for k in range(2):
            hid[:, k * TILE:(k + 1) * TILE] = jnp.maximum(jnp.dot(w1t[...], sbuf[s + k], preferred_element_type=F32), 0.0).astype(BF16)
        pair(acc2, HID, lambda k: hid[:, k * TILE:(k + 1) * TILE], s + 16)
        for k in range(2):
            tile(s + k + 16 + SLOTS).start()
        return 0

    with jax.named_scope('pass2'):
        lax.fori_loop(0, 8, second, 0)

    ut = hid
    with jax.named_scope('wait_m'):
        for c in m_copies:
            c.wait()
    count = jnp.sum(jnp.sum(mall[...], axis=0).astype(F32))
    classes = lax.broadcasted_iota(jnp.int32, (CLS, 512), 0)

    def heads(i, loss):
        cols = pl.ds(pl.multiple_of(i * 512, 512), 512)
        agg = acc2[:, cols].astype(BF16)
        s2t[:, cols] = agg
        z = jnp.dot(w2t[...], agg, preferred_element_type=F32)
        z = jnp.where(classes < 47, z, -1e30)
        z = z - jnp.max(z, axis=0, keepdims=True)
        logp = z - jnp.log(jnp.sum(jnp.exp(z), axis=0, keepdims=True))
        onehot = (label[:, cols] == classes).astype(F32)
        weight = mask[:, cols].astype(F32)
        g2 = (weight * (jnp.exp(logp) - onehot) / count).astype(BF16)
        dcls[:, cols] = g2
        ut[:, cols] = jnp.dot(w2[...], g2, preferred_element_type=F32).astype(BF16)
        return loss + weight * jnp.sum(jnp.where(label[:, cols] == classes, logp, 0.0), axis=0, keepdims=True)

    loss = lax.fori_loop(0, ROWS // 512, heads, jnp.zeros((1, 512), F32))

    to_y = (True, False, False, True, False, True)

    def parts(j, extra):
        if isinstance(j, int) and j < 2:
            return [(pl.ds(0, SUB), j), (pl.ds(SUB, SUB), extra + j)]
        return [(pl.ds(0, TILE), j)]

    def pair_copies(j):
        return [remote(pbuf.at[j % 4, :, cols], rbuf.at[j, :, cols], d_send.at[i], d_recv.at[i], partner)
                for cols, i in parts(j, 8)]

    def link_copies(j):
        return [remote(cbuf.at[j, :, cols], rsbuf.at[j, :, cols], rs_send.at[i], rs_recv.at[i], yn if to_y[j] else xn)
                for cols, i in parts(j, 6)]

    def finalize(j):
        with jax.named_scope('wait_pair'):
            pair_copies(j)[0].wait_recv()
        if j in (4, 5):
            with jax.named_scope('wait_link'):
                for c in link_copies(j - 4):
                    c.wait_recv()
            cbuf[j] = (cbuf[j] + rbuf[j]) + rsbuf[j - 4]
        else:
            cbuf[j] = cbuf[j] + rbuf[j]
        if j < 6:
            link_copies(j)[0].start()

    def sum_copies(red, redp, half, base):
        rows = red.shape[0] // 2
        mine = pl.ds(pl.multiple_of(core * rows, 8), rows)
        links = [remote(half.at[0], half.at[e], f_send.at[base + e], f_recv.at[base + e], dev) for e, dev in ((1, xn), (2, yn), (3, diag))]
        return mine, remote(red, redp, f_send.at[base], f_recv.at[base], partner), links

    mine2, over_chip2, over_chips2 = sum_copies(red2, redp2, half2, 0)
    red2[:CLS, :] = lax.dot_general(dcls[...], s2t[...], LANE_CONTRACT, preferred_element_type=F32)
    red2[CLS:, :] = jnp.broadcast_to(-jnp.sum(loss), (RED2 - CLS, HID))
    over_chip2.start()

    with jax.named_scope('third0'):
        for u in range(32, 36):
            if u > 32:
                tile(u).wait()
        for b in range(2):
            cols = slice(b * SUB, (b + 1) * SUB)
            for q in range(4):
                j = q % 2
                term = jnp.dot(ut[...], ring[q, :, cols], preferred_element_type=F32)
                if q < 2:
                    pbuf[j, :, cols] = term
                    pair_copies(j)[b].start()
                else:
                    cbuf[j, :, cols] = term
                if b == 0 and q == 1:
                    over_chip2.wait()
                    half2[0] = red2[mine2, :] + redp2[mine2, :]
                    for c in over_chips2:
                        c.start()
                if b == 1:
                    tile(32 + q + SLOTS).start()
                if q >= 2:
                    with jax.named_scope('wait_pair'):
                        pair_copies(j)[b].wait_recv()
                    cbuf[j, :, cols] = cbuf[j, :, cols] + rbuf[j, :, cols]
                    link_copies(j)[b].start()

    def wait_sends(j):
        for c in pair_copies(j):
            c.wait_send()

    def third(k, _):
        for q in range(4):
            u, j = 32 + 4 * k + q, 2 * k + q % 2
            tile(u).wait()
            term = jnp.dot(ut[...], ring[u % SLOTS], preferred_element_type=F32)
            if q < 2:
                pl.when(k == 2)(functools.partial(wait_sends, q))
                pl.when(k == 3)(functools.partial(wait_sends, q + 2))
                pbuf[j % 4] = term
                pair_copies(j)[0].start()
            else:
                cbuf[j] = term
            pl.when(k < 2)(tile(u + SLOTS).start)
            if q >= 2:
                for kk in range(1, 4):
                    pl.when(k == kk)(functools.partial(finalize, 2 * kk + q - 2))
        return 0

    with jax.named_scope('pass3'):
        lax.fori_loop(1, 4, third, 0)

    for c in over_chips2:
        c.wait()
    fin2 = pl.ds(pl.multiple_of(RED1 + core * (RED2 // 2), 8), RED2 // 2)
    fin[fin2, :] = (half2[0] + half2[1]) + (half2[2] + half2[3])
    over_pair2 = remote(fin.at[fin2], fin.at[fin2], f_send.at[8], f_recv.at[8], partner)
    over_pair2.start()
    gather_finish(0, xbuf)
    gather_finish(1, sbuf)
    over_pair2.wait()
    for j in range(4, 8):
        wait_sends(j)

    dw1 = jnp.zeros((FEAT, HID), F32)
    for h, (a, b) in enumerate(((3, 4), (2, 5))):
        z1 = jnp.dot(w1t[...], sbuf[h], preferred_element_type=F32)
        with jax.named_scope('wait_own'):
            link_copies(a)[0].wait_recv()
            link_copies(b)[0].wait_recv()
        g1 = jnp.where(z1 > 0.0, (cbuf[6 + h] + rsbuf[a]) + rsbuf[b], 0.0).astype(BF16)
        dw1 = dw1 + lax.dot_general(sbuf[h], g1, LANE_CONTRACT, preferred_element_type=F32)
    red1[:FEAT, :] = dw1
    red1[FEAT:, :] = jnp.zeros((RED1 - FEAT, HID), F32)

    mine1, over_chip1, over_chips1 = sum_copies(red1, redp1, half1, 4)
    with jax.named_scope('sum_chip'):
        over_chip1.start()
        for j in range(6):
            for c in link_copies(j):
                c.wait_send()
        over_chip1.wait()
    half1[0] = red1[mine1, :] + redp1[mine1, :]
    with jax.named_scope('sum_chips'):
        for c in over_chips1:
            c.start()
        for c in over_chips1:
            c.wait()
    fin[mine1, :] = (half1[0] + half1[1]) + (half1[2] + half1[3])
    over_pair1 = remote(fin.at[mine1], fin.at[mine1], f_send.at[9], f_recv.at[9], partner)
    with jax.named_scope('sum_pair'):
        over_pair1.start()
        over_pair1.wait()
    out[:RED1 + CLS, :] = fin[:RED1 + CLS, :]
    out[RED1 + CLS:, :] = fin[RED1 + CLS:, :] / count


def split(total, loss, dw_one, dw_two_t):
    loss[...] = total[RED1 + CLS:RED1 + CLS + 1, :1]
    dw_one[...] = total[:100, :]
    dw_two_t[...] = total[RED1:RED1 + 47, :]


def solution(mesh):
    vmem, anywhere = pl.BlockSpec(memory_space=pltpu.VMEM), pl.BlockSpec(memory_space=pl.ANY)

    def local_step(adj, feat, w_one, w_two, label, mask):
        mask_row = mask.reshape(1, ROWS)
        out = pl.pallas_call(
            kernel,
            out_shape=jax.ShapeDtypeStruct((RED1 + RED2, HID), F32),
            in_specs=[anywhere, anywhere, vmem, vmem, vmem, vmem, anywhere],
            out_specs=vmem,
            scratch_shapes=[
                pltpu.VMEM((HID, FEAT), BF16),
                pltpu.VMEM((CLS, HID), BF16),
                pltpu.VMEM((HID, CLS), BF16),
                pltpu.VMEM((SLOTS, ROWS, TILE), BF16),
                pltpu.VMEM((2, TILE, FLIP), BF16),
                pltpu.VMEM((16, 100, TILE), BF16),
                pltpu.VMEM((16, FEAT, TILE), BF16),
                pltpu.VMEM((FEAT, ROWS), F32),
                pltpu.VMEM((HID, ROWS), F32),
                pltpu.VMEM((HID, ROWS), BF16),
                pltpu.VMEM((HID, ROWS), BF16),
                pltpu.VMEM((8, 1, ROWS), jnp.int32),
                pltpu.VMEM((CLS, ROWS), BF16),
                pltpu.VMEM((4, HID, TILE), F32),
                pltpu.VMEM((8, HID, TILE), F32),
                pltpu.VMEM((8, HID, TILE), F32),
                pltpu.VMEM((6, HID, TILE), F32),
                pltpu.VMEM((RED1, HID), F32),
                pltpu.VMEM((RED1, HID), F32),
                pltpu.VMEM((4, RED1 // 2, HID), F32),
                pltpu.VMEM((RED2, HID), F32),
                pltpu.VMEM((RED2, HID), F32),
                pltpu.VMEM((4, RED2 // 2, HID), F32),
                pltpu.VMEM((RED1 + RED2, HID), F32),
                pltpu.SemaphoreType.DMA((SLOTS,)),
                pltpu.SemaphoreType.DMA((3,)),
                pltpu.SemaphoreType.DMA((2, 16)),
                pltpu.SemaphoreType.DMA((2, 16)),
                pltpu.SemaphoreType.DMA((8,)),
                pltpu.SemaphoreType.DMA((8,)),
                pltpu.SemaphoreType.DMA((10,)),
                pltpu.SemaphoreType.DMA((10,)),
                pltpu.SemaphoreType.DMA((8,)),
                pltpu.SemaphoreType.DMA((8,)),
                pltpu.SemaphoreType.DMA((10,)),
                pltpu.SemaphoreType.DMA((10,)),
            ],
            compiler_params=pltpu.CompilerParams(collective_id=0, has_side_effects=True, vmem_limit_bytes=67043328),
            name='gcn_step',
        )(adj, feat.T, w_one, w_two.T, label.reshape(1, ROWS), mask_row, mask_row)
        loss, dw_one, dw_two_t = pl.pallas_call(
            split,
            out_shape=[jax.ShapeDtypeStruct(shape, F32) for shape in ((1, 1), (100, HID), (47, HID))],
            in_specs=[vmem],
            out_specs=[vmem] * 3,
            name='split',
        )(out)
        return (loss.reshape(1), dw_one, dw_two_t.T)

    return jax.shard_map(local_step, mesh=mesh, in_specs=(P('nodes', None), P('nodes', None), P(None, None), P(None, None), P('nodes'), P('nodes')), out_specs=(P(None), P(None, None), P(None, None)), check_vma=False)
```

```python
import functools

import jax
import jax.numpy as jnp
from jax import lax
from jax.experimental import pallas as pl
from jax.experimental.pallas import tpu as pltpu
from jax.sharding import PartitionSpec as P

MESH = pl.DeviceIdType.MESH
F32, BF16 = jnp.float32, jnp.bfloat16
LANE_CONTRACT = (((1,), (1,)), ((), ()))

ROWS = 2048
TILE = 1024
SLOTS = 8
FLIP = 1280
FEAT = 104
HID = 128
CLS = 48
RED1, RED2 = 112, 64
SUB = TILE // 2


def kernel(adj, feat, w_one, w_two_t, label, mask, mask_any, out,
           w1t, w2t, w2, ring, flip, xbuf, sbuf, acc1, acc2, hid, s2t, mall, dcls,
           pbuf, rbuf, cbuf, rsbuf, red1, redp1, half1, red2, redp2, half2, fin,
           ring_sem, loc_sem, ag_send, ag_recv, m_send, m_recv,
           d_send, d_recv, rs_send, rs_recv, f_send, f_recv):
    me = lax.axis_index('nodes')
    core, px, py = me % 2, (me // 2) % 2, me // 4

    def device(fy, fx, fc):
        return 4 * ((py + fy) % 2) + 2 * ((px + fx) % 2) + (core + fc) % 2

    partner, xn, yn, diag = device(0, 0, 1), device(0, 1, 0), device(1, 0, 0), device(1, 1, 0)

    def columns(u):
        s, back = u % 16, u // 32
        g, r = (1 - back) * (s // 4) + back * (3 - s // 4), s % 2
        fc = (back + (s // 2) % 2) % 2
        t = (g + 1) // 2
        fx, fy = (t + 1 - r) // 2, (t + r) // 2
        h = (r + (g // 2) * (3 - g)) % 2
        return pl.multiple_of(device(fy, fx, fc) * ROWS + h * TILE, TILE)

    def tile(u):
        slot = u % SLOTS
        return pltpu.make_async_copy(adj.at[:, pl.ds(columns(u), TILE)], ring.at[slot], ring_sem.at[slot])

    def remote(src, dst, ssem, rsem, dev):
        return pltpu.make_async_remote_copy(src_ref=src, dst_ref=dst, send_sem=ssem, recv_sem=rsem,
                                            device_id=(dev,), device_id_type=MESH)

    own = [pltpu.make_async_copy(feat.at[:, pl.ds(h * TILE, TILE)], xbuf.at[h], loc_sem.at[h]) for h in range(2)]
    own.append(pltpu.make_async_copy(mask_any, mall.at[0], loc_sem.at[2]))
    for c in own:
        c.start()
    for u in range(3):
        tile(u).start()
    w1t[...] = jnp.concatenate([w_one[...], jnp.zeros((28, HID), F32)], 0).T[:, :FEAT].astype(BF16)
    wide = jnp.concatenate([w_two_t[...], jnp.zeros((81, HID), F32)], 0)
    w2t[...] = wide[:CLS].astype(BF16)
    w2[...] = wide.T[:, :CLS].astype(BF16)
    acc1[...] = jnp.zeros_like(acc1)
    acc2[...] = jnp.zeros_like(acc2)

    peers = [device(e // 4, (e // 2) % 2, e % 2) for e in range(8)]
    barrier = pltpu.get_barrier_semaphore()
    for e in range(1, 8):
        pl.semaphore_signal(barrier, inc=1, device_id=(peers[e],), device_id_type=MESH)
    with jax.named_scope('barrier'):
        pl.semaphore_wait(barrier, 7)

    def gather_copy(ph, buf, src, step, dev):
        return remote(src, buf.at[step], ag_send.at[ph, step], ag_recv.at[ph, step], dev)

    def gather_start(ph, buf, srcs):
        for step, h, dev in ((4, 0, xn), (5, 1, yn), (2, 0, partner), (3, 1, partner), (8, 1, xn), (9, 0, yn)):
            gather_copy(ph, buf, srcs[h], step, dev).start()

    def gather_step(ph, buf, s):
        @pl.when(s >= 2)
        def _():
            gather_copy(ph, buf, buf.at[s], s, partner).wait_recv()

        @pl.when((s >= 4) & (s % 4 < 2))
        def _():
            gather_copy(ph, buf, buf.at[s], s + 2, partner).start()

        for step, dev in ((4, yn), (5, xn)):
            @pl.when(s == step)
            def _(step=step, dev=dev):
                for b in range(2):
                    last_copy(ph, buf, step, step + 8, b, dev).start()

    def last_copy(ph, buf, src, step, b, dev):
        cols = pl.ds(b * SUB, SUB)
        return remote(buf.at[src, :, cols], buf.at[step, :, cols], ag_send.at[ph, step + 4 * b], ag_recv.at[ph, step + 4 * b], dev)

    def gather_finish(ph, buf):
        for step in range(2, 12):
            gather_copy(ph, buf, buf.at[0], step, partner).wait_send()
        for step in range(12, 16):
            for b in range(2):
                last_copy(ph, buf, step, step, b, partner).wait_send()

    for c in own:
        c.wait()
    gather_start(0, xbuf, [xbuf.at[h] for h in range(2)])
    m_copies = [remote(mask_any, mall.at[e], m_send.at[e], m_recv.at[e], peers[e]) for e in range(1, 8)]
    for c in m_copies:
        c.start()

    def flip_rows(u):
        return ring[u % SLOTS, :FLIP, :].T

    def pair(acc, rows, x, u):
        for k in range(2):
            flip[1 - k] = flip_rows(u + k + 1)
            acc[:rows, FLIP:] += lax.dot_general(x(k), ring[(u + k) % SLOTS, FLIP:, :], LANE_CONTRACT, preferred_element_type=F32)
            acc[:rows, :FLIP] += jnp.dot(x(k), flip[k], preferred_element_type=F32)

    def last(acc, rows, ph, buf, x, u, more):
        def flip_half(t, b):
            return ring[(u + t) % SLOTS, :FLIP, b * SUB:(b + 1) * SUB].T

        def wait(t, b):
            last_copy(ph, buf, 12 + t, 12 + t, b, partner).wait_recv()
            if t < 2:
                last_copy(ph, buf, 12 + t, 14 + t, b, partner).start()

        for v in range(u + 5, u + 8):
            tile(v).start()
        for v in range(u + 1, u + 4):
            tile(v).wait()
        flip[0, SUB:, :] = flip_half(1, 0)
        for n, (t0, b) in enumerate(((0, 0), (2, 0), (0, 1), (2, 1))):
            with jax.named_scope('wait_last'):
                wait(t0, b)
                wait(t0 + 1, b)
            now, later = n % 2, 1 - n % 2
            if n == 3 and more:
                tile(u + 4).wait()
                flip[0] = flip_rows(u + 4)
            if n < 3:
                t1, b1 = ((2, 0), (0, 1), (2, 1))[n]
                for t in range(2):
                    flip[later, t * SUB:(t + 1) * SUB, :] = flip_half(t1 + t, b1)
            for t in range(2):
                half = x(t0 + t, b)
                acc[:rows, FLIP:] += lax.dot_general(half, ring[(u + t0 + t) % SLOTS, FLIP:, b * SUB:(b + 1) * SUB], LANE_CONTRACT, preferred_element_type=F32)
                acc[:rows, :FLIP] += jnp.dot(half, flip[now, t * SUB:(t + 1) * SUB, :], preferred_element_type=F32)
        tile(u + 8).start()

    tile(0).wait()
    for u in (3, 4):
        tile(u).start()
    flip[0] = flip_rows(0)

    def first(i, _):
        s = 2 * i
        with jax.named_scope('wait1'):
            for k in range(2):
                tile(s + k + 1).wait()
            for k in range(2):
                tile(s + k + 5).start()
            for k in range(2):
                gather_step(0, xbuf, s + k)
        pair(acc1, 100, lambda k: xbuf[s + k], s)
        return 0

    with jax.named_scope('pass1'):
        lax.fori_loop(0, 6, first, 0)
        last(acc1, 100, 0, xbuf, lambda t, b: xbuf[12 + t, :, b * SUB:(b + 1) * SUB], 12, True)
    for h in range(2):
        sbuf[h] = acc1[:, h * TILE:(h + 1) * TILE].astype(BF16)
    gather_start(1, sbuf, [sbuf.at[h] for h in range(2)])

    def hidden(chunk):
        return jnp.maximum(jnp.dot(w1t[...], chunk, preferred_element_type=F32), 0.0).astype(BF16)

    def second(i, _):
        s = 2 * i
        with jax.named_scope('wait2'):
            tile(s + 17).wait()
            tile(s + 18).wait()
            tile(s + 21).start()
            tile(s + 22).start()
            for k in range(2):
                gather_step(1, sbuf, s + k)
        for k in range(2):
            hid[:, k * TILE:(k + 1) * TILE] = hidden(sbuf[s + k])
        pair(acc2, HID, lambda k: hid[:, k * TILE:(k + 1) * TILE], s + 16)
        return 0

    with jax.named_scope('pass2'):
        lax.fori_loop(0, 6, second, 0)

        def hidden_half(t, b):
            cols = slice(t * SUB, (t + 1) * SUB)
            hid[:, cols] = hidden(sbuf[12 + t, :, b * SUB:(b + 1) * SUB])
            return hid[:, cols]

        last(acc2, HID, 1, sbuf, hidden_half, 28, False)

    ut = hid
    with jax.named_scope('wait_m'):
        for c in m_copies:
            c.wait()
    count = jnp.sum(jnp.sum(mall[...], axis=0).astype(F32))
    classes = lax.broadcasted_iota(jnp.int32, (CLS, 512), 0)

    def heads(i, loss):
        cols = pl.ds(pl.multiple_of(i * 512, 512), 512)
        agg = acc2[:, cols].astype(BF16)
        s2t[:, cols] = agg
        z = jnp.dot(w2t[...], agg, preferred_element_type=F32)
        z = jnp.where(classes < 47, z, -1e30)
        z = z - jnp.max(z, axis=0, keepdims=True)
        logp = z - jnp.log(jnp.sum(jnp.exp(z), axis=0, keepdims=True))
        onehot = (label[:, cols] == classes).astype(F32)
        weight = mask[:, cols].astype(F32)
        g2 = (weight * (jnp.exp(logp) - onehot) / count).astype(BF16)
        dcls[:, cols] = g2
        ut[:, cols] = jnp.dot(w2[...], g2, preferred_element_type=F32).astype(BF16)
        return loss + weight * jnp.sum(jnp.where(label[:, cols] == classes, logp, 0.0), axis=0, keepdims=True)

    loss = lax.fori_loop(0, ROWS // 512, heads, jnp.zeros((1, 512), F32))

    to_y = (True, False, False, True, False, True)

    def parts(j, extra):
        if isinstance(j, int) and j < 2:
            return [(pl.ds(0, SUB), j), (pl.ds(SUB, SUB), extra + j)]
        return [(pl.ds(0, TILE), j)]

    def pair_copies(j):
        return [remote(pbuf.at[j % 4, :, cols], rbuf.at[j, :, cols], d_send.at[i], d_recv.at[i], partner)
                for cols, i in parts(j, 8)]

    def link_copies(j):
        return [remote(cbuf.at[j, :, cols], rsbuf.at[j, :, cols], rs_send.at[i], rs_recv.at[i], yn if to_y[j] else xn)
                for cols, i in parts(j, 6)]

    def finalize(j):
        with jax.named_scope('wait_pair'):
            pair_copies(j)[0].wait_recv()
        if j in (4, 5):
            with jax.named_scope('wait_link'):
                for c in link_copies(j - 4):
                    c.wait_recv()
            cbuf[j] = (cbuf[j] + rbuf[j]) + rsbuf[j - 4]
        else:
            cbuf[j] = cbuf[j] + rbuf[j]
        if j < 6:
            link_copies(j)[0].start()

    def sum_copies(red, redp, half, base):
        rows = red.shape[0] // 2
        mine = pl.ds(pl.multiple_of(core * rows, 8), rows)
        links = [remote(half.at[0], half.at[e], f_send.at[base + e], f_recv.at[base + e], dev) for e, dev in ((1, xn), (2, yn), (3, diag))]
        return mine, remote(red, redp, f_send.at[base], f_recv.at[base], partner), links

    mine2, over_chip2, over_chips2 = sum_copies(red2, redp2, half2, 0)
    red2[:CLS, :] = lax.dot_general(dcls[...], s2t[...], LANE_CONTRACT, preferred_element_type=F32)
    red2[CLS:, :] = jnp.broadcast_to(-jnp.sum(loss), (RED2 - CLS, HID))
    over_chip2.start()

    with jax.named_scope('third0'):
        for u in range(32, 36):
            tile(u).wait()
        for u in range(37, 40):
            tile(u).start()
        for b in range(2):
            cols = slice(b * SUB, (b + 1) * SUB)
            for q in range(4):
                j = q % 2
                term = jnp.dot(ut[...], ring[q, :, cols], preferred_element_type=F32)
                if q < 2:
                    pbuf[j, :, cols] = term
                    pair_copies(j)[b].start()
                else:
                    cbuf[j, :, cols] = term
                if b == 0 and q == 1:
                    over_chip2.wait()
                    half2[0] = red2[mine2, :] + redp2[mine2, :]
                    for c in over_chips2:
                        c.start()
                if b == 1:
                    tile(32 + q + SLOTS).start()
                if q >= 2:
                    with jax.named_scope('wait_pair'):
                        pair_copies(j)[b].wait_recv()
                    cbuf[j, :, cols] = cbuf[j, :, cols] + rbuf[j, :, cols]
                    link_copies(j)[b].start()

    def wait_sends(j):
        for c in pair_copies(j):
            c.wait_send()

    def third(k, _):
        for q in range(4):
            u, j = 32 + 4 * k + q, 2 * k + q % 2
            tile(u).wait()
            term = jnp.dot(ut[...], ring[u % SLOTS], preferred_element_type=F32)
            if q < 2:
                pl.when(k == 2)(functools.partial(wait_sends, q))
                pl.when(k == 3)(functools.partial(wait_sends, q + 2))
                pbuf[j % 4] = term
                pair_copies(j)[0].start()
            else:
                cbuf[j] = term
            pl.when(k < 2)(tile(u + SLOTS).start)
            if q >= 2:
                for kk in range(1, 4):
                    pl.when(k == kk)(functools.partial(finalize, 2 * kk + q - 2))
        return 0

    with jax.named_scope('pass3'):
        lax.fori_loop(1, 4, third, 0)

    for c in over_chips2:
        c.wait()
    fin2 = pl.ds(pl.multiple_of(RED1 + core * (RED2 // 2), 8), RED2 // 2)
    fin[fin2, :] = (half2[0] + half2[1]) + (half2[2] + half2[3])
    over_pair2 = remote(fin.at[fin2], fin.at[fin2], f_send.at[8], f_recv.at[8], partner)
    over_pair2.start()
    gather_finish(0, xbuf)
    gather_finish(1, sbuf)
    over_pair2.wait()
    fin[RED1 + CLS:, :] = fin[RED1 + CLS:, :] / count
    out2 = pltpu.make_async_copy(fin.at[pl.ds(RED1, RED2)], out.at[pl.ds(RED1, RED2)], loc_sem.at[0])
    out2.start()
    for j in range(4, 8):
        wait_sends(j)

    dw1 = jnp.zeros((FEAT, HID), F32)
    for h, (a, b) in enumerate(((3, 4), (2, 5))):
        z1 = jnp.dot(w1t[...], sbuf[h], preferred_element_type=F32)
        with jax.named_scope('wait_own'):
            link_copies(a)[0].wait_recv()
            link_copies(b)[0].wait_recv()
        g1 = jnp.where(z1 > 0.0, (cbuf[6 + h] + rsbuf[a]) + rsbuf[b], 0.0).astype(BF16)
        dw1 = dw1 + lax.dot_general(sbuf[h], g1, LANE_CONTRACT, preferred_element_type=F32)
    red1[:FEAT, :] = dw1
    red1[FEAT:, :] = jnp.zeros((RED1 - FEAT, HID), F32)

    mine1, over_chip1, over_chips1 = sum_copies(red1, redp1, half1, 4)
    with jax.named_scope('sum_chip'):
        over_chip1.start()
        for j in range(6):
            for c in link_copies(j):
                c.wait_send()
        over_chip1.wait()
    half1[0] = red1[mine1, :] + redp1[mine1, :]
    with jax.named_scope('sum_chips'):
        for c in over_chips1:
            c.start()
        for c in over_chips1:
            c.wait()
    fin[mine1, :] = (half1[0] + half1[1]) + (half1[2] + half1[3])
    over_pair1 = remote(fin.at[mine1], out.at[mine1], f_send.at[9], f_recv.at[9], partner)
    with jax.named_scope('sum_pair'):
        over_pair1.start()
        out1 = pltpu.make_async_copy(fin.at[mine1], out.at[mine1], loc_sem.at[1])
        out1.start()
        for c in (out2, out1, over_pair1):
            c.wait()


def split(total, loss, dw_one, dw_two_t):
    loss[...] = total[RED1 + CLS:RED1 + CLS + 1, :1]
    dw_one[...] = total[:100, :]
    dw_two_t[...] = total[RED1:RED1 + 47, :]


def solution(mesh):
    vmem, anywhere = pl.BlockSpec(memory_space=pltpu.VMEM), pl.BlockSpec(memory_space=pl.ANY)

    def local_step(adj, feat, w_one, w_two, label, mask):
        mask_row = mask.reshape(1, ROWS)
        out = pl.pallas_call(
            kernel,
            out_shape=jax.ShapeDtypeStruct((RED1 + RED2, HID), F32),
            in_specs=[anywhere, anywhere, vmem, vmem, vmem, vmem, anywhere],
            out_specs=anywhere,
            scratch_shapes=[
                pltpu.VMEM((HID, FEAT), BF16),
                pltpu.VMEM((CLS, HID), BF16),
                pltpu.VMEM((HID, CLS), BF16),
                pltpu.VMEM((SLOTS, ROWS, TILE), BF16),
                pltpu.VMEM((2, TILE, FLIP), BF16),
                pltpu.VMEM((16, 100, TILE), BF16),
                pltpu.VMEM((16, FEAT, TILE), BF16),
                pltpu.VMEM((FEAT, ROWS), F32),
                pltpu.VMEM((HID, ROWS), F32),
                pltpu.VMEM((HID, ROWS), BF16),
                pltpu.VMEM((HID, ROWS), BF16),
                pltpu.VMEM((8, 1, ROWS), jnp.int32),
                pltpu.VMEM((CLS, ROWS), BF16),
                pltpu.VMEM((4, HID, TILE), F32),
                pltpu.VMEM((8, HID, TILE), F32),
                pltpu.VMEM((8, HID, TILE), F32),
                pltpu.VMEM((6, HID, TILE), F32),
                pltpu.VMEM((RED1, HID), F32),
                pltpu.VMEM((RED1, HID), F32),
                pltpu.VMEM((4, RED1 // 2, HID), F32),
                pltpu.VMEM((RED2, HID), F32),
                pltpu.VMEM((RED2, HID), F32),
                pltpu.VMEM((4, RED2 // 2, HID), F32),
                pltpu.VMEM((RED1 + RED2, HID), F32),
                pltpu.SemaphoreType.DMA((SLOTS,)),
                pltpu.SemaphoreType.DMA((3,)),
                pltpu.SemaphoreType.DMA((2, 20)),
                pltpu.SemaphoreType.DMA((2, 20)),
                pltpu.SemaphoreType.DMA((8,)),
                pltpu.SemaphoreType.DMA((8,)),
                pltpu.SemaphoreType.DMA((10,)),
                pltpu.SemaphoreType.DMA((10,)),
                pltpu.SemaphoreType.DMA((8,)),
                pltpu.SemaphoreType.DMA((8,)),
                pltpu.SemaphoreType.DMA((10,)),
                pltpu.SemaphoreType.DMA((10,)),
            ],
            compiler_params=pltpu.CompilerParams(collective_id=0, has_side_effects=True, vmem_limit_bytes=67043328),
            name='gcn_step',
        )(adj, feat.T, w_one, w_two.T, label.reshape(1, ROWS), mask_row, mask_row)
        loss, dw_one, dw_two_t = pl.pallas_call(
            split,
            out_shape=[jax.ShapeDtypeStruct(shape, F32) for shape in ((1, 1), (100, HID), (47, HID))],
            in_specs=[vmem],
            out_specs=[vmem] * 3,
            name='split',
        )(out)
        return (loss.reshape(1), dw_one, dw_two_t.T)

    return jax.shard_map(local_step, mesh=mesh, in_specs=(P('nodes', None), P('nodes', None), P(None, None), P(None, None), P('nodes'), P('nodes')), out_specs=(P(None), P(None, None), P(None, None)), check_vma=False)
```

```python
import functools

import jax
import jax.numpy as jnp
from jax import lax
from jax.experimental import pallas as pl
from jax.experimental.pallas import tpu as pltpu
from jax.sharding import PartitionSpec as P

MESH = pl.DeviceIdType.MESH
F32, BF16 = jnp.float32, jnp.bfloat16
LANE_CONTRACT = (((1,), (1,)), ((), ()))

ROWS = 2048
TILE = 1024
SLOTS = 6
FLIP = 1280
FEAT = 104
HID = 128
CLS = 48
RED1, RED2 = 112, 64
SUB = TILE // 2


def kernel(adj, feat, w_one_any, w_two_any, label_any, mask_any, out,
           w_one, w_two_t, label, w1t, w2t, w2, ring, flip, xbuf, sbuf, acc1, acc2, hid, s2t, mall, dcls,
           pbuf, rbuf, cbuf, rsbuf, red1, redp1, half1, red2, redp2, half2, fin,
           ring_sem, loc_sem, ag_send, ag_recv, m_send, m_recv,
           d_send, d_recv, rs_send, rs_recv, f_send, f_recv):
    me = lax.axis_index('nodes')
    core, px, py = me % 2, (me // 2) % 2, me // 4

    def device(fy, fx, fc):
        return 4 * ((py + fy) % 2) + 2 * ((px + fx) % 2) + (core + fc) % 2

    partner, xn, yn, diag = device(0, 0, 1), device(0, 1, 0), device(1, 0, 0), device(1, 1, 0)

    def columns(u):
        s, back = u % 16, u // 32
        g, r = (1 - back) * (s // 4) + back * (3 - s // 4), s % 2
        fc = (back + (s // 2) % 2) % 2
        t = (g + 1) // 2
        fx, fy = (t + 1 - r) // 2, (t + r) // 2
        h = (r + (g // 2) * (3 - g)) % 2
        return pl.multiple_of(device(fy, fx, fc) * ROWS + h * TILE, TILE)

    def fetch(u, slot):
        return pltpu.make_async_copy(adj.at[:, pl.ds(columns(u), TILE)], ring.at[slot], ring_sem.at[slot])

    def load(r):
        return fetch(16 * (r // 14) + r % 14 + 2 * (1 - r // 28), r % SLOTS)

    def arrived(slot):
        fetch(0, slot).wait()

    def slot_of(p, s):
        kept = (17 - s) // 16
        return kept * (6 + s) + (1 - kept) * ((4 * (1 - p) + s) % SLOTS)

    def remote(src, dst, ssem, rsem, dev):
        return pltpu.make_async_remote_copy(src_ref=src, dst_ref=dst, send_sem=ssem, recv_sem=rsem,
                                            device_id=(dev,), device_id_type=MESH)

    own = [pltpu.make_async_copy(feat.at[:, pl.ds(h * TILE, TILE)], xbuf.at[h], loc_sem.at[h]) for h in range(2)]
    own.append(pltpu.make_async_copy(mask_any, mall.at[0], loc_sem.at[2]))
    small = [pltpu.make_async_copy(a, b, loc_sem.at[3 + i]) for i, (a, b) in
             enumerate(((w_one_any, w_one), (w_two_any, w_two_t), (label_any, label)))]
    for c in small + own:
        c.start()
    for h in range(2):
        fetch(h, 6 + h).start()
    for r in range(3):
        load(r).start()
    peers = [device(e // 4, (e // 2) % 2, e % 2) for e in range(8)]
    barrier = pltpu.get_barrier_semaphore()
    for e in range(1, 8):
        pl.semaphore_signal(barrier, inc=1, device_id=(peers[e],), device_id_type=MESH)
    for c in small:
        c.wait()
    w1t[...] = jnp.concatenate([w_one[...], jnp.zeros((28, HID), F32)], 0).T[:, :FEAT].astype(BF16)
    wide = jnp.concatenate([w_two_t[...], jnp.zeros((81, HID), F32)], 0)
    w2t[...] = wide[:CLS].astype(BF16)
    w2[...] = wide.T[:, :CLS].astype(BF16)
    acc1[...] = jnp.zeros_like(acc1)
    acc2[...] = jnp.zeros_like(acc2)

    with jax.named_scope('barrier'):
        pl.semaphore_wait(barrier, 7)

    def gather_copy(ph, buf, src, step, dev):
        return remote(src, buf.at[step], ag_send.at[ph, step], ag_recv.at[ph, step], dev)

    def gather_start(ph, buf, srcs):
        for step, h, dev in ((4, 0, xn), (5, 1, yn), (2, 0, partner), (3, 1, partner), (8, 1, xn), (9, 0, yn)):
            gather_copy(ph, buf, srcs[h], step, dev).start()

    def gather_step(ph, buf, s):
        @pl.when(s >= 2)
        def _():
            gather_copy(ph, buf, buf.at[s], s, partner).wait_recv()

        @pl.when((s >= 4) & (s % 4 < 2))
        def _():
            gather_copy(ph, buf, buf.at[s], s + 2, partner).start()

        @pl.when(s == 4)
        def _():
            gather_copy(ph, buf, buf.at[s], 12, yn).start()

        @pl.when(s == 5)
        def _():
            gather_copy(ph, buf, buf.at[s], 13, xn).start()

    def gather_finish(ph, buf):
        for step in range(2, 16):
            gather_copy(ph, buf, buf.at[0], step, partner).wait_send()

    for c in own:
        c.wait()
    gather_start(0, xbuf, [xbuf.at[h] for h in range(2)])
    m_copies = [remote(mask_any, mall.at[e], m_send.at[e], m_recv.at[e], peers[e]) for e in range(1, 8)]
    for c in m_copies:
        c.start()
    for r in range(3, SLOTS):
        load(r).start()

    def flip_rows(slot):
        return ring[slot, :FLIP, :].T

    def pair(acc, rows, x, slots):
        for k in range(2):
            flip[1 - k] = flip_rows(slots[k + 1])
            acc[:rows, FLIP:] += lax.dot_general(x(k), ring[slots[k], FLIP:, :], LANE_CONTRACT, preferred_element_type=F32)
            acc[:rows, :FLIP] += jnp.dot(x(k), flip[k], preferred_element_type=F32)

    arrived(6)
    flip[0] = flip_rows(6)

    def first(i, _):
        s = 2 * i
        slots = [slot_of(0, s), slot_of(0, s + 1), slot_of(0, (s + 2) % 16)]
        with jax.named_scope('wait1'):
            arrived(slots[1])
            pl.when(i < 7)(lambda: arrived(slots[2]))

            @pl.when(i > 1)
            def _():
                for k in range(2):
                    load(s + 2 + k).start()

            for k in range(2):
                gather_step(0, xbuf, s + k)
        pair(acc1, 100, lambda k: xbuf[s + k], slots)
        return 0

    with jax.named_scope('pass1'):
        lax.fori_loop(0, 8, first, 0)
    for h in range(2):
        sbuf[h] = acc1[:, h * TILE:(h + 1) * TILE].astype(BF16)
    gather_start(1, sbuf, [sbuf.at[h] for h in range(2)])

    def second(i, _):
        s = 2 * i
        slots = [slot_of(1, s), slot_of(1, s + 1), slot_of(1, s + 2)]
        with jax.named_scope('wait2'):
            pl.when(i > 0)(lambda: arrived(slots[1]))
            arrived(slots[2])

            @pl.when(i == 0)
            def _():
                for k in range(2):
                    load(18 + k).start()

            @pl.when(i > 1)
            def _():
                for k in range(2):
                    load(s + 16 + k).start()

            for k in range(2):
                gather_step(1, sbuf, s + k)
        for k in range(2):
            hid[:, k * TILE:(k + 1) * TILE] = jnp.maximum(jnp.dot(w1t[...], sbuf[s + k], preferred_element_type=F32), 0.0).astype(BF16)
        pair(acc2, HID, lambda k: hid[:, k * TILE:(k + 1) * TILE], slots)
        return 0

    with jax.named_scope('pass2'):
        lax.fori_loop(0, 8, second, 0)

    ut = hid
    with jax.named_scope('wait_m'):
        for c in m_copies:
            c.wait()
    count = jnp.sum(jnp.sum(mall[...], axis=0).astype(F32))
    classes = lax.broadcasted_iota(jnp.int32, (CLS, 512), 0)

    def heads(i, loss):
        cols = pl.ds(pl.multiple_of(i * 512, 512), 512)
        agg = acc2[:, cols].astype(BF16)
        s2t[:, cols] = agg
        z = jnp.dot(w2t[...], agg, preferred_element_type=F32)
        z = jnp.where(classes < 47, z, -1e30)
        z = z - jnp.max(z, axis=0, keepdims=True)
        logp = z - jnp.log(jnp.sum(jnp.exp(z), axis=0, keepdims=True))
        onehot = (label[:, cols] == classes).astype(F32)
        weight = mall[0, :, cols].astype(F32)
        g2 = (weight * (jnp.exp(logp) - onehot) / count).astype(BF16)
        dcls[:, cols] = g2
        ut[:, cols] = jnp.dot(w2[...], g2, preferred_element_type=F32).astype(BF16)
        return loss + weight * jnp.sum(jnp.where(label[:, cols] == classes, logp, 0.0), axis=0, keepdims=True)

    loss = lax.fori_loop(0, ROWS // 512, heads, jnp.zeros((1, 512), F32))

    to_y = (True, False, False, True, False, True)

    def parts(j, extra):
        if isinstance(j, int) and j < 2:
            return [(pl.ds(0, SUB), j), (pl.ds(SUB, SUB), extra + j)]
        return [(pl.ds(0, TILE), j)]

    def pair_copies(j):
        return [remote(pbuf.at[j % 4, :, cols], rbuf.at[j, :, cols], d_send.at[i], d_recv.at[i], partner)
                for cols, i in parts(j, 8)]

    def link_copies(j):
        return [remote(cbuf.at[j, :, cols], rsbuf.at[j, :, cols], rs_send.at[i], rs_recv.at[i], yn if to_y[j] else xn)
                for cols, i in parts(j, 6)]

    def finalize(j):
        with jax.named_scope('wait_pair'):
            pair_copies(j)[0].wait_recv()
        if j in (4, 5):
            with jax.named_scope('wait_link'):
                for c in link_copies(j - 4):
                    c.wait_recv()
            cbuf[j] = (cbuf[j] + rbuf[j]) + rsbuf[j - 4]
        else:
            cbuf[j] = cbuf[j] + rbuf[j]
        if j < 6:
            link_copies(j)[0].start()

    def sum_copies(red, redp, half, base):
        rows = red.shape[0] // 2
        mine = pl.ds(pl.multiple_of(core * rows, 8), rows)
        links = [remote(half.at[0], half.at[e], f_send.at[base + e], f_recv.at[base + e], dev) for e, dev in ((1, xn), (2, yn), (3, diag))]
        return mine, remote(red, redp, f_send.at[base], f_recv.at[base], partner), links

    mine2, over_chip2, over_chips2 = sum_copies(red2, redp2, half2, 0)
    red2[:CLS, :] = lax.dot_general(dcls[...], s2t[...], LANE_CONTRACT, preferred_element_type=F32)
    red2[CLS:, :] = jnp.broadcast_to(-jnp.sum(loss), (RED2 - CLS, HID))
    over_chip2.start()

    with jax.named_scope('third0'):
        for r in range(29, 32):
            arrived(r % SLOTS)
        for r in (32, 33):
            load(r).start()
        for b in range(2):
            cols = slice(b * SUB, (b + 1) * SUB)
            for q in range(4):
                j = q % 2
                term = jnp.dot(ut[...], ring[(28 + q) % SLOTS, :, cols], preferred_element_type=F32)
                if q < 2:
                    pbuf[j, :, cols] = term
                    pair_copies(j)[b].start()
                else:
                    cbuf[j, :, cols] = term
                if b == 0 and q == 1:
                    over_chip2.wait()
                    half2[0] = red2[mine2, :] + redp2[mine2, :]
                    for c in over_chips2:
                        c.start()
                if b == 1:
                    load(34 + q).start()
                if q >= 2:
                    with jax.named_scope('wait_pair'):
                        pair_copies(j)[b].wait_recv()
                    cbuf[j, :, cols] = cbuf[j, :, cols] + rbuf[j, :, cols]
                    link_copies(j)[b].start()

    def wait_sends(j):
        for c in pair_copies(j):
            c.wait_send()

    def third(k, _):
        for q in range(4):
            r, j, end = 28 + 4 * k + q, 2 * k + q % 2, k // 3
            if q < 2:
                slot = r % SLOTS
                arrived(slot)
            else:
                slot = end * (4 + q) + (1 - end) * (r % SLOTS)
                pl.when(k < 3)(functools.partial(arrived, slot))
            term = jnp.dot(ut[...], ring[slot], preferred_element_type=F32)
            if q < 2:
                pl.when(k == 2)(functools.partial(wait_sends, q))
                pl.when(k == 3)(functools.partial(wait_sends, q + 2))
                pbuf[j % 4] = term
                pair_copies(j)[0].start()
            else:
                cbuf[j] = term
            pl.when(k == 1)(load(r + SLOTS).start)
            if q >= 2:
                for kk in range(1, 4):
                    pl.when(k == kk)(functools.partial(finalize, 2 * kk + q - 2))
        return 0

    with jax.named_scope('pass3'):
        lax.fori_loop(1, 4, third, 0)

    for c in over_chips2:
        c.wait()
    fin2 = pl.ds(pl.multiple_of(RED1 + core * (RED2 // 2), 8), RED2 // 2)
    fin[fin2, :] = (half2[0] + half2[1]) + (half2[2] + half2[3])
    over_pair2 = remote(fin.at[fin2], fin.at[fin2], f_send.at[8], f_recv.at[8], partner)
    over_pair2.start()
    gather_finish(0, xbuf)
    gather_finish(1, sbuf)
    over_pair2.wait()
    fin[RED1 + CLS:, :] = fin[RED1 + CLS:, :] / count
    out2 = pltpu.make_async_copy(fin.at[pl.ds(RED1, RED2)], out.at[pl.ds(RED1, RED2)], loc_sem.at[0])
    out2.start()
    for j in range(4, 8):
        wait_sends(j)

    dw1 = jnp.zeros((FEAT, HID), F32)
    for h, (a, b) in enumerate(((3, 4), (2, 5))):
        z1 = jnp.dot(w1t[...], sbuf[h], preferred_element_type=F32)
        with jax.named_scope('wait_own'):
            link_copies(a)[0].wait_recv()
            link_copies(b)[0].wait_recv()
        g1 = jnp.where(z1 > 0.0, (cbuf[6 + h] + rsbuf[a]) + rsbuf[b], 0.0).astype(BF16)
        dw1 = dw1 + lax.dot_general(sbuf[h], g1, LANE_CONTRACT, preferred_element_type=F32)
    red1[:FEAT, :] = dw1
    red1[FEAT:, :] = jnp.zeros((RED1 - FEAT, HID), F32)

    mine1, over_chip1, over_chips1 = sum_copies(red1, redp1, half1, 4)
    with jax.named_scope('sum_chip'):
        over_chip1.start()
        for j in range(6):
            for c in link_copies(j):
                c.wait_send()
        over_chip1.wait()
    half1[0] = red1[mine1, :] + redp1[mine1, :]
    with jax.named_scope('sum_chips'):
        for c in over_chips1:
            c.start()
        for c in over_chips1:
            c.wait()
    fin[mine1, :] = (half1[0] + half1[1]) + (half1[2] + half1[3])
    over_pair1 = remote(fin.at[mine1], out.at[mine1], f_send.at[9], f_recv.at[9], partner)
    with jax.named_scope('sum_pair'):
        over_pair1.start()
        out1 = pltpu.make_async_copy(fin.at[mine1], out.at[mine1], loc_sem.at[1])
        out1.start()
        for c in (out2, out1, over_pair1):
            c.wait()


def split(total, loss, dw_one, dw_two_t):
    loss[...] = total[RED1 + CLS:RED1 + CLS + 1, :1]
    dw_one[...] = total[:100, :]
    dw_two_t[...] = total[RED1:RED1 + 47, :]


def solution(mesh):
    vmem, anywhere = pl.BlockSpec(memory_space=pltpu.VMEM), pl.BlockSpec(memory_space=pl.ANY)

    def local_step(adj, feat, w_one, w_two, label, mask):
        out = pl.pallas_call(
            kernel,
            out_shape=jax.ShapeDtypeStruct((RED1 + RED2, HID), F32),
            in_specs=[anywhere] * 6,
            out_specs=anywhere,
            scratch_shapes=[
                pltpu.VMEM((100, HID), F32),
                pltpu.VMEM((47, HID), F32),
                pltpu.VMEM((1, ROWS), jnp.int32),
                pltpu.VMEM((HID, FEAT), BF16),
                pltpu.VMEM((CLS, HID), BF16),
                pltpu.VMEM((HID, CLS), BF16),
                pltpu.VMEM((SLOTS + 2, ROWS, TILE), BF16),
                pltpu.VMEM((2, TILE, FLIP), BF16),
                pltpu.VMEM((16, 100, TILE), BF16),
                pltpu.VMEM((16, FEAT, TILE), BF16),
                pltpu.VMEM((FEAT, ROWS), F32),
                pltpu.VMEM((HID, ROWS), F32),
                pltpu.VMEM((HID, ROWS), BF16),
                pltpu.VMEM((HID, ROWS), BF16),
                pltpu.VMEM((8, 1, ROWS), jnp.int32),
                pltpu.VMEM((CLS, ROWS), BF16),
                pltpu.VMEM((4, HID, TILE), F32),
                pltpu.VMEM((8, HID, TILE), F32),
                pltpu.VMEM((8, HID, TILE), F32),
                pltpu.VMEM((6, HID, TILE), F32),
                pltpu.VMEM((RED1, HID), F32),
                pltpu.VMEM((RED1, HID), F32),
                pltpu.VMEM((4, RED1 // 2, HID), F32),
                pltpu.VMEM((RED2, HID), F32),
                pltpu.VMEM((RED2, HID), F32),
                pltpu.VMEM((4, RED2 // 2, HID), F32),
                pltpu.VMEM((RED1 + RED2, HID), F32),
                pltpu.SemaphoreType.DMA((SLOTS + 2,)),
                pltpu.SemaphoreType.DMA((6,)),
                pltpu.SemaphoreType.DMA((2, 16)),
                pltpu.SemaphoreType.DMA((2, 16)),
                pltpu.SemaphoreType.DMA((8,)),
                pltpu.SemaphoreType.DMA((8,)),
                pltpu.SemaphoreType.DMA((10,)),
                pltpu.SemaphoreType.DMA((10,)),
                pltpu.SemaphoreType.DMA((8,)),
                pltpu.SemaphoreType.DMA((8,)),
                pltpu.SemaphoreType.DMA((10,)),
                pltpu.SemaphoreType.DMA((10,)),
            ],
            compiler_params=pltpu.CompilerParams(collective_id=0, has_side_effects=True, vmem_limit_bytes=67043328),
            name='gcn_step',
        )(adj, feat.T, w_one, w_two.T, label.reshape(1, ROWS), mask.reshape(1, ROWS))
        loss, dw_one, dw_two_t = pl.pallas_call(
            split,
            out_shape=[jax.ShapeDtypeStruct(shape, F32) for shape in ((1, 1), (100, HID), (47, HID))],
            in_specs=[vmem],
            out_specs=[vmem] * 3,
            name='split',
        )(out)
        return (loss.reshape(1), dw_one, dw_two_t.T)

    return jax.shard_map(local_step, mesh=mesh, in_specs=(P('nodes', None), P('nodes', None), P(None, None), P(None, None), P('nodes'), P('nodes')), out_specs=(P(None), P(None, None), P(None, None)), check_vma=False)
```

```python
import functools

import jax
import jax.numpy as jnp
from jax import lax
from jax.experimental import pallas as pl
from jax.experimental.pallas import tpu as pltpu
from jax.sharding import PartitionSpec as P

MESH = pl.DeviceIdType.MESH
F32, BF16 = jnp.float32, jnp.bfloat16
LANE_CONTRACT = (((1,), (1,)), ((), ()))

ROWS = 2048
TILE = 1024
SLOTS = 6
FLIP = 1280
FEAT = 104
HID = 128
CLS = 48
RED1, RED2 = 112, 64
SUB = TILE // 2


def kernel(adj, feat, w_one_any, w_two_any, label_any, mask_any, out,
           w_one, w_two_t, label, w1t, w2t, w2, ring, flip, xbuf, sbuf, acc1, acc2, hid, s2t, mall, dcls,
           pbuf, rbuf, cbuf, rsbuf, red1, redp1, half1, red2, redp2, half2, fin,
           ring_sem, loc_sem, ag_send, ag_recv, m_send, m_recv,
           d_send, d_recv, rs_send, rs_recv, f_send, f_recv):
    me = lax.axis_index('nodes')
    core, px, py = me % 2, (me // 2) % 2, me // 4

    def device(fy, fx, fc):
        return 4 * ((py + fy) % 2) + 2 * ((px + fx) % 2) + (core + fc) % 2

    partner, xn, yn, diag = device(0, 0, 1), device(0, 1, 0), device(1, 0, 0), device(1, 1, 0)

    def columns(u):
        s, back = u % 16, u // 32
        g, r = (1 - back) * (s // 4) + back * (3 - s // 4), s % 2
        fc = (back + (s // 2) % 2) % 2
        t = (g + 1) // 2
        fx, fy = (t + 1 - r) // 2, (t + r) // 2
        h = (r + (g // 2) * (3 - g)) % 2
        return pl.multiple_of(device(fy, fx, fc) * ROWS + h * TILE, TILE)

    def fetch(u, slot):
        return pltpu.make_async_copy(adj.at[:, pl.ds(columns(u), TILE)], ring.at[slot], ring_sem.at[slot])

    def load(r):
        return fetch(16 * (r // 14) + r % 14 + 2 * (1 - r // 28), r % SLOTS)

    def arrived(slot):
        fetch(0, slot).wait()

    def slot_of(p, s):
        kept = (17 - s) // 16
        return kept * (6 + s) + (1 - kept) * ((4 * (1 - p) + s) % SLOTS)

    def remote(src, dst, ssem, rsem, dev):
        return pltpu.make_async_remote_copy(src_ref=src, dst_ref=dst, send_sem=ssem, recv_sem=rsem,
                                            device_id=(dev,), device_id_type=MESH)

    own = [pltpu.make_async_copy(feat.at[:, pl.ds(h * TILE, TILE)], xbuf.at[h], loc_sem.at[h]) for h in range(2)]
    own.append(pltpu.make_async_copy(mask_any, mall.at[0], loc_sem.at[2]))
    small = [pltpu.make_async_copy(a, b, loc_sem.at[3 + i]) for i, (a, b) in
             enumerate(((w_one_any, w_one), (w_two_any, w_two_t), (label_any, label)))]
    for c in small + own:
        c.start()
    for h in range(2):
        fetch(h, 6 + h).start()
    for r in range(3):
        load(r).start()
    peers = [device(e // 4, (e // 2) % 2, e % 2) for e in range(8)]
    barrier = pltpu.get_barrier_semaphore()
    for e in range(1, 8):
        pl.semaphore_signal(barrier, inc=1, device_id=(peers[e],), device_id_type=MESH)
    for c in small:
        c.wait()
    w1t[...] = jnp.concatenate([w_one[...], jnp.zeros((28, HID), F32)], 0).T[:, :FEAT].astype(BF16)
    wide = jnp.concatenate([w_two_t[...], jnp.zeros((81, HID), F32)], 0)
    w2t[...] = wide[:CLS].astype(BF16)
    w2[...] = wide.T[:, :CLS].astype(BF16)
    acc1[...] = jnp.zeros_like(acc1)
    acc2[...] = jnp.zeros_like(acc2)

    with jax.named_scope('barrier'):
        pl.semaphore_wait(barrier, 7)

    def gather_copy(ph, buf, src, step, dev):
        return remote(src, buf.at[step], ag_send.at[ph, step], ag_recv.at[ph, step], dev)

    def gather_start(ph, buf, srcs):
        for step, h, dev in ((4, 0, xn), (5, 1, yn), (2, 0, partner), (3, 1, partner), (8, 1, xn), (9, 0, yn)):
            gather_copy(ph, buf, srcs[h], step, dev).start()

    def gather_step(ph, buf, s):
        @pl.when(s >= 2)
        def _():
            gather_copy(ph, buf, buf.at[s], s, partner).wait_recv()

        @pl.when((s >= 4) & (s % 4 < 2))
        def _():
            gather_copy(ph, buf, buf.at[s], s + 2, partner).start()

        @pl.when(s == 4)
        def _():
            gather_copy(ph, buf, buf.at[s], 12, yn).start()

        @pl.when(s == 5)
        def _():
            gather_copy(ph, buf, buf.at[s], 13, xn).start()

    def gather_finish(ph, buf):
        for step in range(2, 16):
            gather_copy(ph, buf, buf.at[0], step, partner).wait_send()

    for c in own:
        c.wait()
    gather_start(0, xbuf, [xbuf.at[h] for h in range(2)])
    m_copies = [remote(mask_any, mall.at[e], m_send.at[e], m_recv.at[e], peers[e]) for e in range(1, 8)]
    for c in m_copies:
        c.start()
    for r in range(3, SLOTS):
        load(r).start()

    def flip_rows(slot):
        return ring[slot, :FLIP, :].T

    def pair(acc, rows, x, slots):
        for k in range(2):
            flip[1 - k] = flip_rows(slots[k + 1])
            acc[:rows, FLIP:] += lax.dot_general(x(k), ring[slots[k], FLIP:, :], LANE_CONTRACT, preferred_element_type=F32)
            acc[:rows, :FLIP] += jnp.dot(x(k), flip[k], preferred_element_type=F32)

    arrived(6)
    flip[0] = flip_rows(6)

    def first(i, _):
        s = 2 * i
        slots = [slot_of(0, s), slot_of(0, s + 1), slot_of(0, (s + 2) % 16)]
        with jax.named_scope('wait1'):
            arrived(slots[1])
            pl.when(i < 7)(lambda: arrived(slots[2]))

            @pl.when(i > 1)
            def _():
                for k in range(2):
                    load(s + 2 + k).start()

            for k in range(2):
                gather_step(0, xbuf, s + k)
        pair(acc1, 100, lambda k: xbuf[s + k], slots)
        return 0

    with jax.named_scope('pass1'):
        lax.fori_loop(0, 8, first, 0)
    for h in range(2):
        sbuf[h] = acc1[:, h * TILE:(h + 1) * TILE].astype(BF16)
    gather_start(1, sbuf, [sbuf.at[h] for h in range(2)])

    def second(i, _):
        s = 2 * i
        slots = [slot_of(1, s), slot_of(1, s + 1), slot_of(1, s + 2)]
        with jax.named_scope('wait2'):
            pl.when(i > 0)(lambda: arrived(slots[1]))
            arrived(slots[2])

            @pl.when(i == 0)
            def _():
                for k in range(2):
                    load(18 + k).start()

            @pl.when(i > 1)
            def _():
                for k in range(2):
                    load(s + 16 + k).start()

            for k in range(2):
                gather_step(1, sbuf, s + k)
        for k in range(2):
            hid[:, k * TILE:(k + 1) * TILE] = jnp.maximum(jnp.dot(w1t[...], sbuf[s + k], preferred_element_type=F32), 0.0).astype(BF16)
        pair(acc2, HID, lambda k: hid[:, k * TILE:(k + 1) * TILE], slots)
        return 0

    with jax.named_scope('pass2'):
        lax.fori_loop(0, 8, second, 0)

    ut = hid
    with jax.named_scope('wait_m'):
        for c in m_copies:
            c.wait()
    count = jnp.sum(jnp.sum(mall[...], axis=0).astype(F32))
    classes = lax.broadcasted_iota(jnp.int32, (CLS, 512), 0)

    def heads(i, loss):
        cols = slice(i * 512, (i + 1) * 512)
        agg = acc2[:, cols].astype(BF16)
        s2t[:, cols] = agg
        z = jnp.dot(w2t[...], agg, preferred_element_type=F32)
        z = jnp.where(classes < 47, z, -1e30)
        z = z - jnp.max(z, axis=0, keepdims=True)
        logp = z - jnp.log(jnp.sum(jnp.exp(z), axis=0, keepdims=True))
        onehot = (label[:, cols] == classes).astype(F32)
        weight = mall[0, :, cols].astype(F32)
        g2 = (weight * (jnp.exp(logp) - onehot) / count).astype(BF16)
        dcls[:, cols] = g2
        ut[:, cols] = jnp.dot(w2[...], g2, preferred_element_type=F32).astype(BF16)
        return loss + weight * jnp.sum(jnp.where(label[:, cols] == classes, logp, 0.0), axis=0, keepdims=True)

    loss = jnp.zeros((1, 512), F32)
    for i in range(ROWS // 512):
        loss = heads(i, loss)

    to_y = (True, False, False, True, False, True)

    def parts(j, extra):
        if isinstance(j, int) and j < 2:
            return [(pl.ds(0, SUB), j), (pl.ds(SUB, SUB), extra + j)]
        return [(pl.ds(0, TILE), j)]

    def pair_copies(j):
        return [remote(pbuf.at[j % 4, :, cols], rbuf.at[j, :, cols], d_send.at[i], d_recv.at[i], partner)
                for cols, i in parts(j, 8)]

    def link_copies(j):
        return [remote(cbuf.at[j, :, cols], rsbuf.at[j, :, cols], rs_send.at[i], rs_recv.at[i], yn if to_y[j] else xn)
                for cols, i in parts(j, 6)]

    def finalize(j):
        with jax.named_scope('wait_pair'):
            pair_copies(j)[0].wait_recv()
        if j in (4, 5):
            with jax.named_scope('wait_link'):
                for c in link_copies(j - 4):
                    c.wait_recv()
            cbuf[j] = (cbuf[j] + rbuf[j]) + rsbuf[j - 4]
        else:
            cbuf[j] = cbuf[j] + rbuf[j]
        if j < 6:
            link_copies(j)[0].start()

    def sum_copies(red, redp, half, base):
        rows = red.shape[0] // 2
        mine = pl.ds(pl.multiple_of(core * rows, 8), rows)
        links = [remote(half.at[0], half.at[e], f_send.at[base + e], f_recv.at[base + e], dev) for e, dev in ((1, xn), (2, yn), (3, diag))]
        return mine, remote(red, redp, f_send.at[base], f_recv.at[base], partner), links

    mine2, over_chip2, over_chips2 = sum_copies(red2, redp2, half2, 0)
    red2[:CLS, :] = lax.dot_general(dcls[...], s2t[...], LANE_CONTRACT, preferred_element_type=F32)
    red2[CLS:, :] = jnp.broadcast_to(-jnp.sum(loss), (RED2 - CLS, HID))
    over_chip2.start()

    with jax.named_scope('third0'):
        for r in range(29, 32):
            arrived(r % SLOTS)
        for r in (32, 33):
            load(r).start()
        for b in range(2):
            cols = slice(b * SUB, (b + 1) * SUB)
            for q in range(4):
                j = q % 2
                term = jnp.dot(ut[...], ring[(28 + q) % SLOTS, :, cols], preferred_element_type=F32)
                if q < 2:
                    pbuf[j, :, cols] = term
                    pair_copies(j)[b].start()
                else:
                    cbuf[j, :, cols] = term
                if b == 0 and q == 1:
                    over_chip2.wait()
                    half2[0] = red2[mine2, :] + redp2[mine2, :]
                    for c in over_chips2:
                        c.start()
                if b == 1:
                    load(34 + q).start()
                if q >= 2:
                    with jax.named_scope('wait_pair'):
                        pair_copies(j)[b].wait_recv()
                    cbuf[j, :, cols] = cbuf[j, :, cols] + rbuf[j, :, cols]
                    link_copies(j)[b].start()

    def wait_sends(j):
        for c in pair_copies(j):
            c.wait_send()

    def third(k, _):
        for q in range(4):
            r, j, end = 28 + 4 * k + q, 2 * k + q % 2, k // 3
            if q < 2:
                slot = r % SLOTS
                arrived(slot)
            else:
                slot = end * (4 + q) + (1 - end) * (r % SLOTS)
                pl.when(k < 3)(functools.partial(arrived, slot))
            term = jnp.dot(ut[...], ring[slot], preferred_element_type=F32)
            if q < 2:
                pl.when(k == 2)(functools.partial(wait_sends, q))
                pl.when(k == 3)(functools.partial(wait_sends, q + 2))
                pbuf[j % 4] = term
                pair_copies(j)[0].start()
            else:
                cbuf[j] = term
            pl.when(k == 1)(load(r + SLOTS).start)
            if q >= 2:
                for kk in range(1, 4):
                    pl.when(k == kk)(functools.partial(finalize, 2 * kk + q - 2))
        return 0

    with jax.named_scope('pass3'):
        lax.fori_loop(1, 4, third, 0)

    for c in over_chips2:
        c.wait()
    fin2 = pl.ds(pl.multiple_of(RED1 + core * (RED2 // 2), 8), RED2 // 2)
    fin[fin2, :] = (half2[0] + half2[1]) + (half2[2] + half2[3])
    over_pair2 = remote(fin.at[fin2], fin.at[fin2], f_send.at[8], f_recv.at[8], partner)
    over_pair2.start()
    gather_finish(0, xbuf)
    gather_finish(1, sbuf)
    over_pair2.wait()
    fin[RED1 + CLS:, :] = fin[RED1 + CLS:, :] / count
    out2 = pltpu.make_async_copy(fin.at[pl.ds(RED1, RED2)], out.at[pl.ds(RED1, RED2)], loc_sem.at[0])
    out2.start()
    for j in range(4, 8):
        wait_sends(j)

    z1 = pbuf
    for h, early in enumerate((3, 2)):
        z1[h] = jnp.dot(w1t[...], sbuf[h], preferred_element_type=F32)
        link_copies(early)[0].wait_recv()
        cbuf[6 + h] = cbuf[6 + h] + rsbuf[early]
    dw1 = jnp.zeros((FEAT, HID), F32)
    for h, late in enumerate((4, 5)):
        with jax.named_scope('wait_own'):
            link_copies(late)[0].wait_recv()
        g1 = jnp.where(z1[h] > 0.0, cbuf[6 + h] + rsbuf[late], 0.0).astype(BF16)
        dw1 = dw1 + lax.dot_general(sbuf[h], g1, LANE_CONTRACT, preferred_element_type=F32)
    red1[:FEAT, :] = dw1
    red1[FEAT:, :] = jnp.zeros((RED1 - FEAT, HID), F32)

    mine1, over_chip1, over_chips1 = sum_copies(red1, redp1, half1, 4)
    with jax.named_scope('sum_chip'):
        over_chip1.start()
        for j in range(6):
            for c in link_copies(j):
                c.wait_send()
        over_chip1.wait()
    half1[0] = red1[mine1, :] + redp1[mine1, :]
    with jax.named_scope('sum_chips'):
        for c in over_chips1:
            c.start()
        for c in over_chips1:
            c.wait()
    fin[mine1, :] = (half1[0] + half1[1]) + (half1[2] + half1[3])
    over_pair1 = remote(fin.at[mine1], out.at[mine1], f_send.at[9], f_recv.at[9], partner)
    with jax.named_scope('sum_pair'):
        over_pair1.start()
        out1 = pltpu.make_async_copy(fin.at[mine1], out.at[mine1], loc_sem.at[1])
        out1.start()
        for c in (out2, out1, over_pair1):
            c.wait()


def split(total, loss, dw_one, dw_two_t):
    loss[...] = total[RED1 + CLS:RED1 + CLS + 1, :1]
    dw_one[...] = total[:100, :]
    dw_two_t[...] = total[RED1:RED1 + 47, :]


def solution(mesh):
    vmem, anywhere = pl.BlockSpec(memory_space=pltpu.VMEM), pl.BlockSpec(memory_space=pl.ANY)

    def local_step(adj, feat, w_one, w_two, label, mask):
        out = pl.pallas_call(
            kernel,
            out_shape=jax.ShapeDtypeStruct((RED1 + RED2, HID), F32),
            in_specs=[anywhere] * 6,
            out_specs=anywhere,
            scratch_shapes=[
                pltpu.VMEM((100, HID), F32),
                pltpu.VMEM((47, HID), F32),
                pltpu.VMEM((1, ROWS), jnp.int32),
                pltpu.VMEM((HID, FEAT), BF16),
                pltpu.VMEM((CLS, HID), BF16),
                pltpu.VMEM((HID, CLS), BF16),
                pltpu.VMEM((SLOTS + 2, ROWS, TILE), BF16),
                pltpu.VMEM((2, TILE, FLIP), BF16),
                pltpu.VMEM((16, 100, TILE), BF16),
                pltpu.VMEM((16, FEAT, TILE), BF16),
                pltpu.VMEM((FEAT, ROWS), F32),
                pltpu.VMEM((HID, ROWS), F32),
                pltpu.VMEM((HID, ROWS), BF16),
                pltpu.VMEM((HID, ROWS), BF16),
                pltpu.VMEM((8, 1, ROWS), jnp.int32),
                pltpu.VMEM((CLS, ROWS), BF16),
                pltpu.VMEM((4, HID, TILE), F32),
                pltpu.VMEM((8, HID, TILE), F32),
                pltpu.VMEM((8, HID, TILE), F32),
                pltpu.VMEM((6, HID, TILE), F32),
                pltpu.VMEM((RED1, HID), F32),
                pltpu.VMEM((RED1, HID), F32),
                pltpu.VMEM((4, RED1 // 2, HID), F32),
                pltpu.VMEM((RED2, HID), F32),
                pltpu.VMEM((RED2, HID), F32),
                pltpu.VMEM((4, RED2 // 2, HID), F32),
                pltpu.VMEM((RED1 + RED2, HID), F32),
                pltpu.SemaphoreType.DMA((SLOTS + 2,)),
                pltpu.SemaphoreType.DMA((6,)),
                pltpu.SemaphoreType.DMA((2, 16)),
                pltpu.SemaphoreType.DMA((2, 16)),
                pltpu.SemaphoreType.DMA((8,)),
                pltpu.SemaphoreType.DMA((8,)),
                pltpu.SemaphoreType.DMA((10,)),
                pltpu.SemaphoreType.DMA((10,)),
                pltpu.SemaphoreType.DMA((8,)),
                pltpu.SemaphoreType.DMA((8,)),
                pltpu.SemaphoreType.DMA((10,)),
                pltpu.SemaphoreType.DMA((10,)),
            ],
            compiler_params=pltpu.CompilerParams(collective_id=0, has_side_effects=True, vmem_limit_bytes=67043328),
            name='gcn_step',
        )(adj, feat.T, w_one, w_two.T, label.reshape(1, ROWS), mask.reshape(1, ROWS))
        loss, dw_one, dw_two_t = pl.pallas_call(
            split,
            out_shape=[jax.ShapeDtypeStruct(shape, F32) for shape in ((1, 1), (100, HID), (47, HID))],
            in_specs=[vmem],
            out_specs=[vmem] * 3,
            name='split',
        )(out)
        return (loss.reshape(1), dw_one, dw_two_t.T)

    return jax.shard_map(local_step, mesh=mesh, in_specs=(P('nodes', None), P('nodes', None), P(None, None), P(None, None), P('nodes'), P('nodes')), out_specs=(P(None), P(None, None), P(None, None)), check_vma=False)
```
